8 devices in a mesh: dp: 1 (over z), tp: 2 (over y), ep: 4 (over x, core).
Axes of the slice: x: 2, y: 2, z: 1, core: 2. Of those that a mesh axis runs over, the one named last changes fastest.
Arguments:
- tokens_x: bfloat16 [1024, 2048], P(('dp', 'ep', 'tp'))
- expert_ids: int32 [1024, 2], P(('dp', 'ep', 'tp'))
- route_gate: float32 [1024, 2], P(('dp', 'ep', 'tp'))
- w_gate: bfloat16 [8, 2048, 5632], P('ep', None, 'tp')
- w_up: bfloat16 [8, 2048, 5632], P('ep', None, 'tp')
- w_down: bfloat16 [8, 5632, 2048], P('ep', 'tp')
Outputs:
- output: bfloat16 [1024, 2048], P(('dp', 'ep', 'tp'))
All inputs are finite; a program needn't handle non-finite values.
Results may differ from the reference program's by a relative error of at most 0.00124.
Values are sent between devices in bfloat16 or wider.
A program may use at most 1 GiB of HBM per device.

```python
import jax
import jax.numpy as jnp
from jax import lax

D_MODEL = 2048
FF_DIM = 5632
EXPERTS = 8
TOP_K = 2
EP_GROUP = 4
TOKENS = 1024


def draw_routing(route_key):
    num_blocks = TOKENS // EXPERTS
    per_dev = EXPERTS // EP_GROUP
    key_pos, key_dev, key_loc = jax.random.split(route_key, 3)
    row_pos = jax.vmap(lambda one_key: jax.random.permutation(one_key, EXPERTS))(jax.random.split(key_pos, num_blocks))
    dev_perm = jax.vmap(lambda one_key: jax.random.permutation(one_key, EP_GROUP))(jax.random.split(key_dev, num_blocks))
    loc_perm = jax.vmap(lambda one_key: jax.random.permutation(one_key, per_dev))(jax.random.split(key_loc, num_blocks * EP_GROUP))
    loc_perm = loc_perm.reshape(num_blocks, EP_GROUP, per_dev)
    slot_offset = jnp.arange(TOP_K, dtype=jnp.int32)

    def block_ids(dev_order, loc_order, positions):
        labels = (positions[:, None] + slot_offset[None, :]) % EXPERTS
        dev_slot = labels % EP_GROUP
        return dev_order[dev_slot] * per_dev + loc_order[dev_slot, labels // EP_GROUP]

    all_ids = jax.vmap(block_ids)(dev_perm, loc_perm, row_pos)
    return all_ids.reshape(TOKENS, TOP_K).astype(jnp.int32)


def setup_inputs(seed: int = 0, part: int = 0) -> dict:
    part_key = jax.random.fold_in(jax.random.key(seed), part)
    key_x, key_gate, key_route = jax.random.split(part_key, 3)
    key_wg, key_wu, key_wd = jax.random.split(jax.random.key(seed + 1), 3)
    tokens_x = jax.random.normal(key_x, (TOKENS, D_MODEL), jnp.float32).astype(jnp.bfloat16)
    expert_ids = draw_routing(key_route)
    route_gate = jax.random.uniform(key_gate, (TOKENS, TOP_K), jnp.float32, 0.5, 1.5) * TOP_K ** -0.5
    w_gate = (jax.random.normal(key_wg, (EXPERTS, D_MODEL, FF_DIM), jnp.float32) * D_MODEL ** -0.5).astype(jnp.bfloat16)
    w_up = (jax.random.normal(key_wu, (EXPERTS, D_MODEL, FF_DIM), jnp.float32) * D_MODEL ** -0.5).astype(jnp.bfloat16)
    w_down = (jax.random.normal(key_wd, (EXPERTS, FF_DIM, D_MODEL), jnp.float32) * FF_DIM ** -0.5).astype(jnp.bfloat16)
    return dict(tokens_x=tokens_x, expert_ids=expert_ids, route_gate=route_gate, w_gate=w_gate, w_up=w_up, w_down=w_down)


def reference(tokens_x, expert_ids, route_gate, w_gate, w_up, w_down):
    expert_cap = TOKENS * TOP_K // EXPERTS
    sort_order = jnp.argsort(expert_ids.reshape(-1), stable=True)
    tok_rows = (sort_order // TOP_K).reshape(EXPERTS, expert_cap)
    gate_rows = route_gate.reshape(-1)[sort_order].reshape(EXPERTS, expert_cap)

    def add_expert(acc_sum, per_expert):
        rows_e, gates_e, wg_e, wu_e, wd_e = per_expert
        x_rows = tokens_x[rows_e]
        h_gate = jnp.dot(x_rows, wg_e, preferred_element_type=jnp.float32)
        h_up = jnp.dot(x_rows, wu_e, preferred_element_type=jnp.float32)
        hidden = (jax.nn.silu(h_gate) * h_up).astype(jnp.bfloat16)
        out_rows = jnp.dot(hidden, wd_e, preferred_element_type=jnp.float32) * gates_e[:, None]
        return acc_sum.at[rows_e].add(out_rows), None

    acc_init = jnp.zeros((TOKENS, D_MODEL), jnp.float32)
    y_total, _ = lax.scan(add_expert, acc_init, (tok_rows, gate_rows, w_gate, w_up, w_down))
    return y_total.astype(jnp.bfloat16)
```

```python
import functools

import jax
import jax.numpy as jnp
from jax import lax
from jax.experimental import pallas as pl
from jax.experimental.pallas import tpu as pltpu
from jax.sharding import PartitionSpec as P

MESH = pl.DeviceIdType.MESH
BF16 = jnp.bfloat16
F32 = jnp.float32
CW = 256


def moe_kernel(ids_ref, gate_ref, x_ref, wg_hbm, wu_hbm, wd_hbm, y_ref,
               gbuf, ubuf, dbuf, xbuf, sendbuf, hbuf, obuf, ybuf, hy, hx, psend, precv, dacc,
               ids_p, gate_p, sel, gsel,
               gsem, usem, dsem, xs_sem, xr_sem, aux_s, aux_r,
               ys_sem, yr_sem, x1s_sem, x1r_sem, y2s_sem, y2r_sem, ps_sem, pr_sem):
    n_gu = gbuf.shape[0]
    n_cc = ybuf.shape[1]
    slots = sendbuf.shape[1]
    ep = lax.axis_index('ep')
    tp = lax.axis_index('tp')
    other_tp = 1 - tp
    me = tp * 4 + ep

    def dev(e, t):
        return {'ep': e, 'tp': t}

    peers = [(dt, de) for dt in (0, 1) for de in range(4) if (dt, de) != (0, 0)]

    def peer(dt, de):
        return lax.rem(ep + de, 4), lax.rem(tp + dt, 2)

    def gu_copy(p, j):
        cols = pl.ds(pl.multiple_of(j * CW, CW), CW)
        return (pltpu.make_async_copy(wg_hbm.at[p, :, cols], gbuf.at[j], gsem.at[j]),
                pltpu.make_async_copy(wu_hbm.at[p, :, cols], ubuf.at[j], usem.at[j]))

    def d_copy(p, c):
        cols = pl.ds(pl.multiple_of(c * CW, CW), CW)
        return pltpu.make_async_copy(wd_hbm.at[p, :, cols], dbuf.at[c], dsem.at[c])

    @pl.loop(0, n_gu)
    def _(j):
        a, b = gu_copy(0, j)
        a.start()
        b.start()

    @pl.loop(0, 2 * n_cc)
    def _(c):
        d_copy(0, c).start()

    barrier = pltpu.get_barrier_semaphore()
    for dt, de in peers:
        e, t = peer(dt, de)
        pl.semaphore_signal(barrier, inc=1, device_id=dev(e, t), device_id_type=MESH)

    def slot_of(ids):
        ids = ids[...]
        e_iota = lax.broadcasted_iota(jnp.int32, (16, 128), 0)
        one0 = jnp.where(e_iota == ids[0:1, :], 1.0, 0.0).astype(F32)
        one1 = jnp.where(e_iota == ids[1:2, :], 1.0, 0.0).astype(F32)
        before = jnp.where(lax.broadcasted_iota(jnp.int32, (128, 128), 0)
                           < lax.broadcasted_iota(jnp.int32, (128, 128), 1), 1.0, 0.0)
        count = jnp.dot((one0 + one1).astype(BF16), before.astype(BF16), preferred_element_type=F32)
        rank0 = jnp.sum(one0 * count, axis=0, keepdims=True).astype(jnp.int32)
        rank1 = jnp.sum(one1 * count, axis=0, keepdims=True).astype(jnp.int32)
        return ids[0:1, :] * slots + rank0, ids[1:2, :] * slots + rank1

    def build(which, ids, gates):
        pos0, pos1 = slot_of(ids)
        k_iota = lax.broadcasted_iota(jnp.int32, (8 * slots, 128), 0)
        hit0 = jnp.where(k_iota == pos0, 1.0, 0.0).astype(F32)
        hit1 = jnp.where(k_iota == pos1, 1.0, 0.0).astype(F32)
        picked = hit0 * gates[0:1, :] + hit1 * gates[1:2, :]
        gsel[which] = jnp.broadcast_to(jnp.sum(picked, axis=1, keepdims=True), (8 * slots, CW))
        both = hit0 + hit1
        sel[which] = both.T.astype(BF16)
        return both.astype(BF16)

    gather = build(0, ids_ref, gate_ref)
    sorted_rows = jnp.dot(gather, x_ref[...], preferred_element_type=F32).astype(BF16)
    sendbuf[...] = sorted_rows.reshape(sendbuf.shape)

    pl.semaphore_wait(barrier, 7)

    def aux_copies():
        return (pltpu.make_async_remote_copy(ids_ref, ids_p, aux_s.at[0], aux_r.at[0],
                                             device_id=dev(ep, other_tp), device_id_type=MESH),
                pltpu.make_async_remote_copy(gate_ref, gate_p, aux_s.at[1], aux_r.at[1],
                                             device_id=dev(ep, other_tp), device_id_type=MESH))

    for copy in aux_copies():
        copy.start()

    def row_copy(p, i, src_home):
        dt, de = peers[i]
        e, t = peer(dt, de)
        return pltpu.make_async_remote_copy(
            sendbuf.at[2 * e + p], xbuf.at[p, src_home], xs_sem.at[p, i], xr_sem.at[p, src_home],
            device_id=dev(e, t), device_id_type=MESH)

    for p in range(2):
        for i in range(7):
            row_copy(p, i, me).start()
        xbuf[p, me] = sendbuf[2 * ep + p]

    def o_view(p, c):
        return obuf.at[p, c]

    def y1_copy(p, cc):
        return pltpu.make_async_remote_copy(
            obuf.at[p, 2 * cc, other_tp], ybuf.at[p, cc], ys_sem.at[p, cc], yr_sem.at[p, cc],
            device_id=dev(ep, other_tp), device_id_type=MESH)

    def x1_copy(p, cc, de, src_ep):
        he = lax.rem(ep + de, 4)
        return pltpu.make_async_remote_copy(
            obuf.at[p, 2 * cc + 1, :, he], hx.at[cc, :, 2 * src_ep + p],
            x1s_sem.at[p, cc, de - 1], x1r_sem.at[p, cc, src_ep],
            device_id=dev(he, tp), device_id_type=MESH)

    def y2_copy(p, cc, de, src_ep):
        he = lax.rem(ep + de, 4)
        return pltpu.make_async_remote_copy(
            ybuf.at[p, cc, he], hy.at[cc, 2 * src_ep + p],
            y2s_sem.at[p, cc, de - 1], y2r_sem.at[p, cc, src_ep],
            device_id=dev(he, tp), device_id_type=MESH)

    def p_copy(cc):
        return pltpu.make_async_remote_copy(
            psend.at[cc], precv.at[cc], ps_sem.at[cc], pr_sem.at[cc],
            device_id=dev(ep, other_tp), device_id_type=MESH)

    rows = 8 * slots
    for p in range(2):
        for dt, de in peers:
            e, t = peer(dt, de)
            pltpu.make_async_remote_copy(
                sendbuf.at[p], xbuf.at[p, t * 4 + e], xs_sem.at[p, 0], xr_sem.at[p, t * 4 + e],
                device_id=dev(e, t), device_id_type=MESH).wait_recv()

        @pl.loop(0, n_gu)
        def _(j):
            a, b = gu_copy(p, j)
            a.wait()
            b.wait()
            xs = xbuf[p].reshape(rows, xbuf.shape[-1])
            g = jnp.dot(xs, gbuf[j], preferred_element_type=F32)
            u = jnp.dot(xs, ubuf[j], preferred_element_type=F32)
            hbuf[:, pl.ds(pl.multiple_of(j * CW, CW), CW)] = (jax.nn.silu(g) * u).astype(BF16)
            if p == 0:
                a, b = gu_copy(1, j)
                a.start()
                b.start()

        @pl.loop(0, n_cc)
        def _(cc):
            d_copy(p, 2 * cc).wait()
            o = jnp.dot(hbuf[...], dbuf[2 * cc], preferred_element_type=F32)
            obuf[p, 2 * cc] = o.reshape(obuf.shape[2:])
            if p == 0:
                d_copy(1, 2 * cc).start()
            y1_copy(p, cc).start()
            d_copy(p, 2 * cc + 1).wait()
            o = jnp.dot(hbuf[...], dbuf[2 * cc + 1], preferred_element_type=F32)
            obuf[p, 2 * cc + 1] = o.reshape(obuf.shape[2:])
            if p == 0:
                d_copy(1, 2 * cc + 1).start()
            for de in (1, 2, 3):
                x1_copy(p, cc, de, ep).start()
            hx[cc, :, 2 * ep + p] = obuf[p, 2 * cc + 1, :, ep]

    for copy in aux_copies():
        copy.wait_recv()
    build(1, ids_p, gate_p)

    def scatter(which, values):
        v = values.reshape(rows, CW) * gsel[which]
        hi = v.astype(BF16)
        rest = v - hi.astype(F32)
        mid = rest.astype(BF16)
        low = (rest - mid.astype(F32)).astype(BF16)
        s = sel[which]
        return (jnp.dot(s, low, preferred_element_type=F32)
                + jnp.dot(s, mid, preferred_element_type=F32)
                + jnp.dot(s, hi, preferred_element_type=F32))

    @pl.loop(0, n_cc)
    def _(cc):
        for p in range(2):
            y1_copy(p, cc).wait_recv()
            ybuf[p, cc] = ybuf[p, cc] + obuf[p, 2 * cc, tp]
            for de in (1, 2, 3):
                y2_copy(p, cc, de, ep).start()
            hy[cc, 2 * ep + p] = ybuf[p, cc, ep]
        for p in range(2):
            for de in (1, 2, 3):
                x1_copy(p, cc, de, lax.rem(ep + de, 4)).wait_recv()
        psend[cc] = scatter(1, hx[cc, other_tp])
        p_copy(cc).start()
        dacc[cc] = scatter(0, hx[cc, tp])

    @pl.loop(0, n_cc)
    def _(cc):
        for p in range(2):
            for de in (1, 2, 3):
                y2_copy(p, cc, de, lax.rem(ep + de, 4)).wait_recv()
        y_ref[:, pl.ds(pl.multiple_of(2 * cc * CW, CW), CW)] = scatter(0, hy[cc]).astype(y_ref.dtype)
        p_copy(cc).wait_recv()
        y_ref[:, pl.ds(pl.multiple_of((2 * cc + 1) * CW, CW), CW)] = (dacc[cc] + precv[cc]).astype(y_ref.dtype)

    for copy in aux_copies():
        copy.wait_send()
    for p in range(2):
        for i in range(7):
            row_copy(p, i, me).wait_send()

        @pl.loop(0, n_cc)
        def _(cc):
            y1_copy(p, cc).wait_send()
            for de in (1, 2, 3):
                x1_copy(p, cc, de, ep).wait_send()
                y2_copy(p, cc, de, ep).wait_send()

    @pl.loop(0, n_cc)
    def _(cc):
        p_copy(cc).wait_send()


def solution(mesh):
    row_spec = P(('dp', 'ep', 'tp'), None)
    w_in_spec = P('ep', None, 'tp')
    w_out_spec = P('ep', 'tp', None)

    def local_moe(x_local, ids_local, gate_local, w_gate, w_up, w_down):
        n_rows, d_model = x_local.shape
        ff = w_gate.shape[2]
        slots = 2 * n_rows // 8
        n_gu = ff // CW
        n_cc = d_model // CW // 2
        dma = pltpu.SemaphoreType.DMA
        vmem = pl.BlockSpec(memory_space=pltpu.VMEM)
        hbm = pl.BlockSpec(memory_space=pl.ANY)
        return pl.pallas_call(
            moe_kernel,
            out_shape=jax.ShapeDtypeStruct((n_rows, d_model), BF16),
            in_specs=[vmem, vmem, vmem, hbm, hbm, hbm],
            out_specs=vmem,
            scratch_shapes=[
                pltpu.VMEM((n_gu, d_model, CW), BF16),
                pltpu.VMEM((n_gu, d_model, CW), BF16),
                pltpu.VMEM((2 * n_cc, ff, CW), BF16),
                pltpu.VMEM((2, 8, slots, d_model), BF16),
                pltpu.VMEM((8, slots, d_model), BF16),
                pltpu.VMEM((8 * slots, ff), BF16),
                pltpu.VMEM((2, 2 * n_cc, 2, 4, slots, CW), F32),
                pltpu.VMEM((2, n_cc, 4, slots, CW), F32),
                pltpu.VMEM((n_cc, 8, slots, CW), F32),
                pltpu.VMEM((n_cc, 2, 8, slots, CW), F32),
                pltpu.VMEM((n_cc, n_rows, CW), F32),
                pltpu.VMEM((n_cc, n_rows, CW), F32),
                pltpu.VMEM((n_cc, n_rows, CW), F32),
                pltpu.VMEM((2, n_rows), jnp.int32),
                pltpu.VMEM((2, n_rows), F32),
                pltpu.VMEM((2, n_rows, 8 * slots), BF16),
                pltpu.VMEM((2, 8 * slots, CW), F32),
                dma((n_gu,)), dma((n_gu,)), dma((2 * n_cc,)),
                dma((2, 7)), dma((2, 8)), dma((2,)), dma((2,)),
                dma((2, n_cc)), dma((2, n_cc)),
                dma((2, n_cc, 3)), dma((2, n_cc, 4)),
                dma((2, n_cc, 3)), dma((2, n_cc, 4)),
                dma((n_cc,)), dma((n_cc,)),
            ],
            compiler_params=pltpu.CompilerParams(
                collective_id=0, has_side_effects=True, vmem_limit_bytes=60 * 1024 * 1024),
        )(ids_local.T, gate_local.T, x_local, w_gate, w_up, w_down)

    return jax.shard_map(local_moe, mesh=mesh,
                         in_specs=(row_spec, row_spec, row_spec, w_in_spec, w_in_spec, w_out_spec),
                         out_specs=row_spec, check_vma=False)
```

```python
import jax
import jax.numpy as jnp
from jax import lax
from jax.experimental import pallas as pl
from jax.experimental.pallas import tpu as pltpu
from jax.sharding import PartitionSpec as P

MESH = pl.DeviceIdType.MESH
BF16 = jnp.bfloat16
F32 = jnp.float32
CW = 256
NY = 2


def moe_kernel(ids_ref, gate_ref, x_hbm, wg_hbm, wu_hbm, wd_hbm, y_ref,
               xin, gubuf, dbuf, xbuf, sendbuf, hbuf, obuf, ybuf, hy, hx, psend, precv, dacc,
               ids_p, gate_p, sel, gsel,
               xin_sem, gsem, usem, dsem, xs_sem, xr_sem, aux_s, aux_r,
               ys_sem, yr_sem, x1s_sem, x1r_sem, y2s_sem, y2r_sem, ps_sem, pr_sem):
    n_gu = gubuf.shape[0]
    n_c = dbuf.shape[0]
    n_x = n_c - NY
    slots = sendbuf.shape[1]
    rows = 8 * slots
    half = 4 * slots
    ep = lax.axis_index('ep')
    tp = lax.axis_index('tp')
    tq = 1 - tp
    ec = ep + 1 - 2 * lax.rem(ep, 2)
    ex = lax.rem(ep + 2, 4)
    exc = lax.rem(ec + 2, 4)

    def dev(e, t):
        return {'ep': e, 'tp': t}

    def cols(j):
        return pl.ds(pl.multiple_of(j * CW, CW), CW)

    def remote(src, dst, send, recv, e, t):
        return pltpu.make_async_remote_copy(src, dst, send, recv, device_id=dev(e, t), device_id_type=MESH)

    x_copy = pltpu.make_async_copy(x_hbm, xin, xin_sem)
    x_copy.start()

    def gu_copies(p, j):
        return (pltpu.make_async_copy(wg_hbm.at[p, :, cols(j)], gubuf.at[j, :, pl.ds(0, CW)], gsem.at[j]),
                pltpu.make_async_copy(wu_hbm.at[p, :, cols(j)], gubuf.at[j, :, pl.ds(CW, CW)], usem.at[j]))

    def d_copy(p, c):
        return pltpu.make_async_copy(wd_hbm.at[p, :, cols(c)], dbuf.at[c], dsem.at[c])

    def start_gu(p):
        @pl.loop(0, n_gu)
        def _(j):
            for copy in gu_copies(p, j):
                copy.start()

    def start_d(p):
        @pl.loop(0, n_c)
        def _(c):
            d_copy(p, c).start()

    start_gu(0)
    start_d(0)

    barrier = pltpu.get_barrier_semaphore()
    for dt in (0, 1):
        for de in range(4):
            if (dt, de) != (0, 0):
                pl.semaphore_signal(barrier, inc=1, device_id=dev(lax.rem(ep + de, 4), lax.rem(tp + dt, 2)),
                                    device_id_type=MESH)

    def slot_of(ids):
        ids = ids[...]
        e_iota = lax.broadcasted_iota(jnp.int32, (16, 128), 0)
        one0 = jnp.where(e_iota == ids[0:1, :], 1.0, 0.0).astype(F32)
        one1 = jnp.where(e_iota == ids[1:2, :], 1.0, 0.0).astype(F32)
        before = jnp.where(lax.broadcasted_iota(jnp.int32, (128, 128), 0)
                           < lax.broadcasted_iota(jnp.int32, (128, 128), 1), 1.0, 0.0)
        count = jnp.dot((one0 + one1).astype(BF16), before.astype(BF16), preferred_element_type=F32)
        rank0 = jnp.sum(one0 * count, axis=0, keepdims=True).astype(jnp.int32)
        rank1 = jnp.sum(one1 * count, axis=0, keepdims=True).astype(jnp.int32)
        return ids[0:1, :] * slots + rank0, ids[1:2, :] * slots + rank1

    def build(which, ids, gates):
        pos0, pos1 = slot_of(ids)
        k_iota = lax.broadcasted_iota(jnp.int32, (rows, 128), 0)
        hit0 = jnp.where(k_iota == pos0, 1.0, 0.0).astype(F32)
        hit1 = jnp.where(k_iota == pos1, 1.0, 0.0).astype(F32)
        picked = hit0 * gates[0:1, :] + hit1 * gates[1:2, :]
        gsel[which] = jnp.broadcast_to(jnp.sum(picked, axis=1, keepdims=True), (rows, CW))
        both = hit0 + hit1
        sel[which] = both.T.astype(BF16)
        return both.astype(BF16)

    gather = build(0, ids_ref, gate_ref)
    x_copy.wait()
    sorted_rows = jnp.dot(gather, xin[...], preferred_element_type=F32).astype(BF16)
    sendbuf[...] = sorted_rows.reshape(sendbuf.shape)
    for p in range(2):
        xbuf[p, tp, ep] = sendbuf[2 * ep + p]

    pl.semaphore_wait(barrier, 7)

    def row_copy(p, k):
        e, t = ((ex, tp), (exc, tp), (ep, tq), (ec, tq), (ec, tp))[k]
        return remote(sendbuf.at[2 * e + p], xbuf.at[p, tp, ep], xs_sem.at[p, k], xr_sem.at[p, tp, ep], e, t)

    def relay_copy(p, k):
        home = (ex, exc)[k]
        return remote(xbuf.at[p, tp, home], xbuf.at[p, tp, home], xs_sem.at[p, 5 + k], xr_sem.at[p, tp, home],
                      ep, tq)

    def wait_rows(p, th, he):
        remote(sendbuf.at[0], xbuf.at[p, th, he], xs_sem.at[0, 0], xr_sem.at[p, th, he], ep, tq).wait_recv()

    def aux_copies():
        return (remote(ids_ref, ids_p, aux_s.at[0], aux_r.at[0], ep, tq),
                remote(gate_ref, gate_p, aux_s.at[1], aux_r.at[1], ep, tq))

    for k in range(5):
        row_copy(0, k).start()
    for k in (0, 1, 4):
        row_copy(1, k).start()
    for copy in aux_copies():
        copy.start()
    for k in range(2):
        wait_rows(0, tp, (ex, exc)[k])
        relay_copy(0, k).start()
    for k in (2, 3):
        row_copy(1, k).start()
    wait_rows(0, tp, ec)

    def y1_copy(p, cy):
        return remote(obuf.at[p, tq, cy], ybuf.at[p, cy], ys_sem.at[p, cy], yr_sem.at[p, cy], ep, tq)

    def x1_copy(p, g, cx, de, src_ep):
        th = tp + g * (1 - 2 * tp)
        he = lax.rem(ep + de, 4)
        return remote(obuf.at[p, th, NY + cx, he], hx.at[g, cx, 2 * src_ep + p],
                      x1s_sem.at[p, g, cx, de - 1], x1r_sem.at[p, g, cx, src_ep], he, tp)

    def y2_copy(p, cy, de, src_ep):
        he = lax.rem(ep + de, 4)
        return remote(ybuf.at[p, cy, he], hy.at[cy, 2 * src_ep + p],
                      y2s_sem.at[p, cy, de - 1], y2r_sem.at[p, cy, src_ep], he, tp)

    def p_copy(cx):
        return remote(psend.at[cx], precv.at[cx], ps_sem.at[cx], pr_sem.at[cx], ep, tq)

    @pl.loop(0, 4)
    def _(s):
        p = s // 2
        g = lax.rem(s + 1, 4) // 2
        th = tp + g * (1 - 2 * tp)

        @pl.when(s == 1)
        def _():
            for k in range(2):
                wait_rows(1, tp, (ex, exc)[k])
                relay_copy(1, k).start()
            for he in range(4):
                wait_rows(0, tq, he)

        @pl.when(s == 2)
        def _():
            for copy in aux_copies():
                copy.wait_recv()
            build(1, ids_p, gate_p)
            for he in range(4):
                wait_rows(1, tq, he)
            wait_rows(1, tp, ec)

        @pl.when(lax.rem(s, 2) == 0)
        def _():
            @pl.loop(0, n_gu)
            def _(j):
                for copy in gu_copies(p, j):
                    copy.wait()

        xs = xbuf[p, th].reshape(half, xin.shape[1])
        for j in range(n_gu):
            ab = jnp.dot(xs, gubuf[j], preferred_element_type=F32)
            a, b = ab[:, :CW], ab[:, CW:]
            hbuf[:, j * CW:(j + 1) * CW] = (jax.nn.silu(a) * b).astype(BF16)

        @pl.when(s == 1)
        def _():
            start_gu(1)

        @pl.when(lax.rem(s, 2) == 0)
        def _():
            @pl.loop(0, n_c)
            def _(c):
                d_copy(p, c).wait()

        def down(c):
            o = jnp.dot(hbuf[...], dbuf[c], preferred_element_type=F32)
            obuf[p, th, c] = o.reshape(4, slots, CW)

        def send_x(c):
            for de in (2, 3, 1):
                x1_copy(p, g, c - NY, de, ep).start()
            hx[g, c - NY, 2 * ep + p] = obuf[p, th, c, ep]

        for c in range(4):
            down(c)

        @pl.when(g == 1)
        def _():
            for cy in range(NY):
                y1_copy(p, cy).start()

        for c in range(NY, 4):
            send_x(c)
        for c in range(4, n_c):
            down(c)
        for c in range(4, n_c):
            send_x(c)

        @pl.when(s == 1)
        def _():
            start_d(1)

    def scatter(which, values):
        v = values.reshape(rows, CW) * gsel[which]
        hi = v.astype(BF16)
        rest = v - hi.astype(F32)
        mid = rest.astype(BF16)
        low = (rest - mid.astype(F32)).astype(BF16)
        s = sel[which]
        return (jnp.dot(s, low, preferred_element_type=F32)
                + jnp.dot(s, mid, preferred_element_type=F32)
                + jnp.dot(s, hi, preferred_element_type=F32))

    def wait_x(g, cx):
        for p in range(2):
            for de in (1, 2, 3):
                x1_copy(p, g, cx, de, lax.rem(ep + de, 4)).wait_recv()

    def send_p(cx):
        wait_x(1, cx)
        psend[cx] = scatter(1, hx[1, cx])
        p_copy(cx).start()

    send_p(0)
    send_p(1)

    @pl.loop(0, NY)
    def _(cy):
        for p in range(2):
            y1_copy(p, cy).wait_recv()
            ybuf[p, cy] = ybuf[p, cy] + obuf[p, tp, cy]
            for de in (2, 3, 1):
                y2_copy(p, cy, de, ep).start()
            hy[cy, 2 * ep + p] = ybuf[p, cy, ep]

    @pl.loop(2, n_x)
    def _(cx):
        send_p(cx)

    @pl.loop(0, n_x)
    def _(cx):
        wait_x(0, cx)
        dacc[cx] = scatter(0, hx[0, cx])

    @pl.loop(0, n_x - 1)
    def _(cx):
        p_copy(cx).wait_recv()
        y_ref[:, cols(NY + cx)] = (dacc[cx] + precv[cx]).astype(y_ref.dtype)

    @pl.loop(0, NY)
    def _(cy):
        for p in range(2):
            for de in (1, 2, 3):
                y2_copy(p, cy, de, lax.rem(ep + de, 4)).wait_recv()
        y_ref[:, cols(cy)] = scatter(0, hy[cy]).astype(y_ref.dtype)

    p_copy(n_x - 1).wait_recv()
    y_ref[:, cols(n_c - 1)] = (dacc[n_x - 1] + precv[n_x - 1]).astype(y_ref.dtype)

    for copy in aux_copies():
        copy.wait_send()
    for p in range(2):
        for k in range(5):
            row_copy(p, k).wait_send()
        for k in range(2):
            relay_copy(p, k).wait_send()

        @pl.loop(0, NY)
        def _(cy):
            y1_copy(p, cy).wait_send()
            for de in (1, 2, 3):
                y2_copy(p, cy, de, ep).wait_send()

        for g in range(2):
            @pl.loop(0, n_x)
            def _(cx):
                for de in (1, 2, 3):
                    x1_copy(p, g, cx, de, ep).wait_send()

    @pl.loop(0, n_x)
    def _(cx):
        p_copy(cx).wait_send()


def solution(mesh):
    row_spec = P(('dp', 'ep', 'tp'), None)
    w_in_spec = P('ep', None, 'tp')
    w_out_spec = P('ep', 'tp', None)

    def local_moe(x_local, ids_local, gate_local, w_gate, w_up, w_down):
        n_rows, d_model = x_local.shape
        ff = w_gate.shape[2]
        slots = 2 * n_rows // 8
        n_gu = ff // CW
        n_c = d_model // CW
        n_x = n_c - NY
        dma = pltpu.SemaphoreType.DMA
        vmem = pl.BlockSpec(memory_space=pltpu.VMEM)
        hbm = pl.BlockSpec(memory_space=pltpu.HBM)
        return pl.pallas_call(
            moe_kernel,
            out_shape=jax.ShapeDtypeStruct((n_rows, d_model), BF16),
            in_specs=[vmem, vmem, hbm, hbm, hbm, hbm],
            out_specs=vmem,
            scratch_shapes=[
                pltpu.VMEM((n_rows, d_model), BF16),
                pltpu.VMEM((n_gu, d_model, 2 * CW), BF16),
                pltpu.VMEM((n_c, ff, CW), BF16),
                pltpu.VMEM((2, 2, 4, slots, d_model), BF16),
                pltpu.VMEM((8, slots, d_model), BF16),
                pltpu.VMEM((4 * slots, ff), BF16),
                pltpu.VMEM((2, 2, n_c, 4, slots, CW), F32),
                pltpu.VMEM((2, NY, 4, slots, CW), F32),
                pltpu.VMEM((NY, 8, slots, CW), F32),
                pltpu.VMEM((2, n_x, 8, slots, CW), F32),
                pltpu.VMEM((n_x, n_rows, CW), F32),
                pltpu.VMEM((n_x, n_rows, CW), F32),
                pltpu.VMEM((n_x, n_rows, CW), F32),
                pltpu.VMEM((2, n_rows), jnp.int32),
                pltpu.VMEM((2, n_rows), F32),
                pltpu.VMEM((2, n_rows, 8 * slots), BF16),
                pltpu.VMEM((2, 8 * slots, CW), F32),
                dma, dma((n_gu,)), dma((n_gu,)), dma((n_c,)),
                dma((2, 7)), dma((2, 2, 4)), dma((2,)), dma((2,)),
                dma((2, NY)), dma((2, NY)),
                dma((2, 2, n_x, 3)), dma((2, 2, n_x, 4)),
                dma((2, NY, 3)), dma((2, NY, 4)),
                dma((n_x,)), dma((n_x,)),
            ],
            compiler_params=pltpu.CompilerParams(
                collective_id=0, has_side_effects=True, vmem_limit_bytes=52 * 1024 * 1024),
        )(ids_local.T, gate_local.T, x_local, w_gate, w_up, w_down)

    return jax.shard_map(local_moe, mesh=mesh,
                         in_specs=(row_spec, row_spec, row_spec, w_in_spec, w_in_spec, w_out_spec),
                         out_specs=row_spec, check_vma=False)
```

```python
import jax
import jax.numpy as jnp
from jax import lax
from jax.experimental import pallas as pl
from jax.experimental.pallas import tpu as pltpu
from jax.sharding import PartitionSpec as P

MESH = pl.DeviceIdType.MESH
BF16 = jnp.bfloat16
F32 = jnp.float32
CW = 256
NY = 2


def moe_kernel(ids_hbm, gate_hbm, x_hbm, wg_hbm, wu_hbm, wd_hbm, y_ref,
               ids_ref, gate_ref, xin, gubuf, dbuf, xbuf, sendbuf, hbuf, obuf, ybuf, hy, hx, psend, precv, dacc,
               ids_p, gate_p, sel, gsel,
               in_sem, gu_sem, d_sem, xs_sem, xr_sem, aux_s, aux_r,
               y1_sem, x1s_sem, x1r_sem, y2s_sem, y2r_sem, ps_sem, pr_sem):
    n_gu = gubuf.shape[0]
    n_c = dbuf.shape[0]
    n_x = n_c - NY
    slots = sendbuf.shape[1]
    rows = 8 * slots
    half = 4 * slots
    ep = lax.axis_index('ep')
    tp = lax.axis_index('tp')
    tq = 1 - tp
    ec = ep + 1 - 2 * lax.rem(ep, 2)
    ex = lax.rem(ep + 2, 4)
    exc = lax.rem(ec + 2, 4)

    def dev(e, t):
        return {'ep': e, 'tp': t}

    def cols(j):
        return pl.ds(pl.multiple_of(j * CW, CW), CW)

    def remote(src, dst, send, recv, e, t):
        return pltpu.make_async_remote_copy(src, dst, send, recv, device_id=dev(e, t), device_id_type=MESH)

    in_copies = [pltpu.make_async_copy(src, dst, in_sem.at[i])
                 for i, (src, dst) in enumerate(((ids_hbm, ids_ref), (gate_hbm, gate_ref), (x_hbm, xin)))]
    for copy in in_copies:
        copy.start()

    def gu_copies(p, j):
        return (pltpu.make_async_copy(wg_hbm.at[p, :, cols(j)], gubuf.at[j, :, pl.ds(0, CW)], gu_sem),
                pltpu.make_async_copy(wu_hbm.at[p, :, cols(j)], gubuf.at[j, :, pl.ds(CW, CW)], gu_sem))

    def d_copy(p, c):
        return pltpu.make_async_copy(wd_hbm.at[p, :, cols(c)], dbuf.at[c], d_sem)

    def start_gu(p):
        @pl.loop(0, n_gu)
        def _(j):
            for copy in gu_copies(p, j):
                copy.start()

    def start_d(p):
        @pl.loop(0, n_c)
        def _(c):
            d_copy(p, c).start()

    start_gu(0)
    start_d(0)

    barrier = pltpu.get_barrier_semaphore()
    partners = ((ex, tp), (exc, tp), (ep, tq), (ec, tq), (ec, tp))
    for e, t in partners:
        pl.semaphore_signal(barrier, inc=1, device_id=dev(e, t), device_id_type=MESH)

    def slot_of(ids):
        ids = ids[...]
        e_iota = lax.broadcasted_iota(jnp.int32, (16, 128), 0)
        one0 = jnp.where(e_iota == ids[0:1, :], 1.0, 0.0).astype(F32)
        one1 = jnp.where(e_iota == ids[1:2, :], 1.0, 0.0).astype(F32)
        before = jnp.where(lax.broadcasted_iota(jnp.int32, (128, 128), 0)
                           < lax.broadcasted_iota(jnp.int32, (128, 128), 1), 1.0, 0.0)
        count = jnp.dot((one0 + one1).astype(BF16), before.astype(BF16), preferred_element_type=F32)
        rank0 = jnp.sum(one0 * count, axis=0, keepdims=True).astype(jnp.int32)
        rank1 = jnp.sum(one1 * count, axis=0, keepdims=True).astype(jnp.int32)
        return ids[0:1, :] * slots + rank0, ids[1:2, :] * slots + rank1

    def build(which, ids, gates):
        pos0, pos1 = slot_of(ids)
        k_iota = lax.broadcasted_iota(jnp.int32, (rows, 128), 0)
        hit0 = jnp.where(k_iota == pos0, 1.0, 0.0).astype(F32)
        hit1 = jnp.where(k_iota == pos1, 1.0, 0.0).astype(F32)
        picked = hit0 * gates[0:1, :] + hit1 * gates[1:2, :]
        gsel[which] = jnp.broadcast_to(jnp.sum(picked, axis=1, keepdims=True), (rows, CW))
        both = hit0 + hit1
        sel[which] = both.T.astype(BF16)
        return both.astype(BF16)

    in_copies[0].wait()
    in_copies[1].wait()
    gather = build(0, ids_ref, gate_ref)
    in_copies[2].wait()
    sorted_rows = jnp.dot(gather, xin[...], preferred_element_type=F32).astype(BF16)
    sendbuf[...] = sorted_rows.reshape(sendbuf.shape)
    for p in range(2):
        xbuf[p, tp, ep] = sendbuf[2 * ep + p]

    pl.semaphore_wait(barrier, 5)

    def row_copy(p, k):
        e, t = partners[k]
        return remote(sendbuf.at[2 * e + p], xbuf.at[p, tp, ep], xs_sem.at[p], xr_sem.at[p, (1, 2, 0, 0, 3)[k]], e, t)

    def relay_copy(p, k):
        home = (ex, exc)[k]
        return remote(xbuf.at[p, tp, home], xbuf.at[p, tp, home], xs_sem.at[2], xr_sem.at[p, 0], ep, tq)

    def wait_rows(p, k):
        ref = xbuf.at[p, tq] if k == 0 else xbuf.at[p, tp, (ex, exc, ec)[k - 1]]
        remote(ref, ref, xs_sem.at[0], xr_sem.at[p, k], ep, tq).wait_recv()

    def aux_copies():
        return (remote(ids_ref, ids_p, aux_s.at[0], aux_r.at[0], ep, tq),
                remote(gate_ref, gate_p, aux_s.at[1], aux_r.at[1], ep, tq))

    for k in range(5):
        row_copy(0, k).start()
    for k in (0, 1, 4):
        row_copy(1, k).start()
    for copy in aux_copies():
        copy.start()
    for k in range(2):
        wait_rows(0, 1 + k)
        relay_copy(0, k).start()
    for k in (2, 3):
        row_copy(1, k).start()
    wait_rows(0, 3)

    def y1_copy(p, cy):
        return remote(obuf.at[p, tq, cy], ybuf.at[p, cy], y1_sem.at[0], y1_sem.at[1], ep, tq)

    def x1_copy(p, g, cx, de, src_ep):
        th = tp + g * (1 - 2 * tp)
        he = lax.rem(ep + de, 4)
        return remote(obuf.at[p, th, NY + cx, he], hx.at[g, cx, 2 * src_ep + p],
                      x1s_sem, x1r_sem.at[g, cx], he, tp)

    def y2_copy(p, cy, de, src_ep):
        he = lax.rem(ep + de, 4)
        return remote(ybuf.at[p, cy, he], hy.at[cy, 2 * src_ep + p],
                      y2s_sem, y2r_sem.at[cy], he, tp)

    def p_copy(cx):
        return remote(psend.at[cx], precv.at[cx], ps_sem, pr_sem.at[cx], ep, tq)

    @pl.loop(0, 4)
    def _(s):
        p = s // 2
        g = lax.rem(s + 1, 4) // 2
        th = tp + g * (1 - 2 * tp)

        @pl.when(s == 1)
        def _():
            for k in range(2):
                wait_rows(1, 1 + k)
                relay_copy(1, k).start()
            wait_rows(0, 0)

        @pl.when(s == 2)
        def _():
            for copy in aux_copies():
                copy.wait_recv()
            build(1, ids_p, gate_p)
            wait_rows(1, 0)
            wait_rows(1, 3)

        @pl.when(lax.rem(s, 2) == 0)
        def _():
            pltpu.make_async_copy(gubuf, gubuf, gu_sem).wait()

        xs = xbuf[p, th].reshape(half, xin.shape[1])
        for j in range(n_gu):
            ab = jnp.dot(xs, gubuf[j], preferred_element_type=F32)
            a, b = ab[:, :CW], ab[:, CW:]
            hbuf[:, j * CW:(j + 1) * CW] = (jax.nn.silu(a) * b).astype(BF16)

        @pl.when(s == 1)
        def _():
            start_gu(1)

        @pl.when(lax.rem(s, 2) == 0)
        def _():
            pltpu.make_async_copy(dbuf, dbuf, d_sem).wait()

        def down(c):
            o = jnp.dot(hbuf[...], dbuf[c], preferred_element_type=F32)
            obuf[p, th, c] = o.reshape(4, slots, CW)

        def send_x(c):
            for de in (2, 3, 1):
                x1_copy(p, g, c - NY, de, ep).start()
            hx[g, c - NY, 2 * ep + p] = obuf[p, th, c, ep]

        for c in range(NY):
            down(c)

        @pl.when(g == 1)
        def _():
            for cy in range(NY):
                y1_copy(p, cy).start()

        mid = (NY + n_c) // 2
        for part in (range(NY, mid), range(mid, n_c)):
            for c in part:
                down(c)
            for c in part:
                send_x(c)

        @pl.when(s == 1)
        def _():
            start_d(1)

    def scatter(which, values):
        v = values.reshape(rows, CW) * gsel[which]
        hi = v.astype(BF16)
        rest = v - hi.astype(F32)
        mid = rest.astype(BF16)
        low = (rest - mid.astype(F32)).astype(BF16)
        s = sel[which]
        return (jnp.dot(s, low, preferred_element_type=F32)
                + jnp.dot(s, mid, preferred_element_type=F32)
                + jnp.dot(s, hi, preferred_element_type=F32))

    def wait_x(g, cx):
        six = hx.at[g, cx, pl.ds(0, 6)]
        remote(six, six, x1s_sem, x1r_sem.at[g, cx], ep, tq).wait_recv()

    def send_p(cx):
        wait_x(1, cx)
        psend[cx] = scatter(1, hx[1, cx])
        p_copy(cx).start()

    send_p(0)
    send_p(1)

    remote(ybuf, ybuf, y1_sem.at[0], y1_sem.at[1], ep, tq).wait_recv()

    @pl.loop(0, NY)
    def _(cy):
        for p in range(2):
            ybuf[p, cy] = ybuf[p, cy] + obuf[p, tp, cy]
            for de in (2, 3, 1):
                y2_copy(p, cy, de, ep).start()
            hy[cy, 2 * ep + p] = ybuf[p, cy, ep]

    @pl.loop(2, n_x)
    def _(cx):
        send_p(cx)

    @pl.loop(0, n_x)
    def _(cx):
        wait_x(0, cx)
        dacc[cx] = scatter(0, hx[0, cx])

    @pl.loop(0, n_x - 1)
    def _(cx):
        p_copy(cx).wait_recv()
        y_ref[:, cols(NY + cx)] = (dacc[cx] + precv[cx]).astype(y_ref.dtype)

    @pl.loop(0, NY)
    def _(cy):
        six = hy.at[cy, pl.ds(0, 6)]
        remote(six, six, y2s_sem, y2r_sem.at[cy], ep, tq).wait_recv()
        y_ref[:, cols(cy)] = scatter(0, hy[cy]).astype(y_ref.dtype)

    p_copy(n_x - 1).wait_recv()
    y_ref[:, cols(n_c - 1)] = (dacc[n_x - 1] + precv[n_x - 1]).astype(y_ref.dtype)

    for copy in aux_copies():
        copy.wait_send()
    for p in range(2):
        five = sendbuf.at[pl.ds(0, 5)]
        remote(five, five, xs_sem.at[p], xr_sem.at[0, 0], ep, tq).wait_send()
    four = xbuf.at[0, 0]
    remote(four, four, xs_sem.at[2], xr_sem.at[0, 0], ep, tq).wait_send()
    remote(ybuf, ybuf, y1_sem.at[0], y1_sem.at[1], ep, tq).wait_send()
    sent = hx.at[:, :, pl.ds(0, 6)]
    remote(sent, sent, x1s_sem, x1r_sem.at[0, 0], ep, tq).wait_send()
    sent = hy.at[:, pl.ds(0, 6)]
    remote(sent, sent, y2s_sem, y2r_sem.at[0], ep, tq).wait_send()
    remote(psend, psend, ps_sem, pr_sem.at[0], ep, tq).wait_send()


def solution(mesh):
    row_spec = P(('dp', 'ep', 'tp'), None)
    w_in_spec = P('ep', None, 'tp')
    w_out_spec = P('ep', 'tp', None)

    def local_moe(x_local, ids_local, gate_local, w_gate, w_up, w_down):
        n_rows, d_model = x_local.shape
        ff = w_gate.shape[2]
        slots = 2 * n_rows // 8
        n_gu = ff // CW
        n_c = d_model // CW
        n_x = n_c - NY
        dma = pltpu.SemaphoreType.DMA
        vmem = pl.BlockSpec(memory_space=pltpu.VMEM)
        hbm = pl.BlockSpec(memory_space=pltpu.HBM)
        return pl.pallas_call(
            moe_kernel,
            out_shape=jax.ShapeDtypeStruct((n_rows, d_model), BF16),
            in_specs=[hbm] * 6,
            out_specs=vmem,
            scratch_shapes=[
                pltpu.VMEM((2, n_rows), jnp.int32),
                pltpu.VMEM((2, n_rows), F32),
                pltpu.VMEM((n_rows, d_model), BF16),
                pltpu.VMEM((n_gu, d_model, 2 * CW), BF16),
                pltpu.VMEM((n_c, ff, CW), BF16),
                pltpu.VMEM((2, 2, 4, slots, d_model), BF16),
                pltpu.VMEM((8, slots, d_model), BF16),
                pltpu.VMEM((4 * slots, ff), BF16),
                pltpu.VMEM((2, 2, n_c, 4, slots, CW), F32),
                pltpu.VMEM((2, NY, 4, slots, CW), F32),
                pltpu.VMEM((NY, 8, slots, CW), F32),
                pltpu.VMEM((2, n_x, 8, slots, CW), F32),
                pltpu.VMEM((n_x, n_rows, CW), F32),
                pltpu.VMEM((n_x, n_rows, CW), F32),
                pltpu.VMEM((n_x, n_rows, CW), F32),
                pltpu.VMEM((2, n_rows), jnp.int32),
                pltpu.VMEM((2, n_rows), F32),
                pltpu.VMEM((2, n_rows, 8 * slots), BF16),
                pltpu.VMEM((2, 8 * slots, CW), F32),
                dma((3,)), dma, dma,
                dma((3,)), dma((2, 4)), dma((2,)), dma((2,)),
                dma((2,)), dma, dma((2, n_x)),
                dma, dma((NY,)), dma, dma((n_x,)),
            ],
            compiler_params=pltpu.CompilerParams(
                collective_id=0, has_side_effects=True, vmem_limit_bytes=52 * 1024 * 1024),
        )(*(pltpu.with_memory_space_constraint(a, pltpu.HBM) for a in (ids_local.T, gate_local.T, x_local)),
          w_gate, w_up, w_down)

    return jax.shard_map(local_moe, mesh=mesh,
                         in_specs=(row_spec, row_spec, row_spec, w_in_spec, w_in_spec, w_out_spec),
                         out_specs=row_spec, check_vma=False)
```

```python
import jax
import jax.numpy as jnp
from jax import lax
from jax.experimental import pallas as pl
from jax.experimental.pallas import tpu as pltpu
from jax.sharding import PartitionSpec as P

MESH = pl.DeviceIdType.MESH
BF16 = jnp.bfloat16
F32 = jnp.float32
CW = 256
NY = 2


def moe_kernel(ids_hbm, gate_hbm, x_hbm, wg_hbm, wu_hbm, wd_hbm, y_ref,
               ids_ref, gate_ref, xin, gubuf, dbuf, xbuf, sendbuf, hbuf, obuf, ybuf, hy, hx, psend, precv, dacc,
               ids_p, gate_p, sel, gsel,
               in_sem, gu_sem, d_sem, xs_sem, xr_sem, aux_s, aux_r,
               y1_sem, x1s_sem, x1r_sem, y2s_sem, y2r_sem, ps_sem, pr_sem):
    n_gu = gubuf.shape[0]
    n_c = dbuf.shape[0]
    n_x = n_c - NY
    slots = sendbuf.shape[1]
    rows = 8 * slots
    half = 4 * slots
    ep = lax.axis_index('ep')
    tp = lax.axis_index('tp')
    tq = 1 - tp
    ec = ep + 1 - 2 * lax.rem(ep, 2)
    ex = lax.rem(ep + 2, 4)
    exc = lax.rem(ec + 2, 4)

    def dev(e, t):
        return {'ep': e, 'tp': t}

    def cols(j):
        return pl.ds(pl.multiple_of(j * CW, CW), CW)

    def remote(src, dst, send, recv, e, t):
        return pltpu.make_async_remote_copy(src, dst, send, recv, device_id=dev(e, t), device_id_type=MESH)

    barrier = pltpu.get_barrier_semaphore()
    partners = ((ex, tp), (exc, tp), (ep, tq), (ec, tq), (ec, tp))
    for e, t in partners:
        pl.semaphore_signal(barrier, inc=1, device_id=dev(e, t), device_id_type=MESH)

    in_copies = [pltpu.make_async_copy(src, dst, in_sem.at[i])
                 for i, (src, dst) in enumerate(((ids_hbm, ids_ref), (gate_hbm, gate_ref), (x_hbm, xin)))]
    for copy in in_copies:
        copy.start()

    def gu_copies(p, j, seg):
        return (pltpu.make_async_copy(wg_hbm.at[p, :, cols(j)], gubuf.at[j, :, pl.ds(0, CW)], gu_sem.at[seg]),
                pltpu.make_async_copy(wu_hbm.at[p, :, cols(j)], gubuf.at[j, :, pl.ds(CW, CW)], gu_sem.at[seg]))

    gu_segs = ((0, 4), (4, 8), (8, n_gu))
    d_segs = ((NY, NY + 1), (NY + 1, n_c), (0, NY))

    def start_gu(p, seg):
        @pl.loop(*gu_segs[seg])
        def _(j):
            for copy in gu_copies(p, j, seg):
                copy.start()

    def wait_gu(seg):
        lo, hi = gu_segs[seg]
        ref = gubuf.at[pl.ds(lo, hi - lo)]
        pltpu.make_async_copy(ref, ref, gu_sem.at[seg]).wait()

    def start_d(p, seg):
        for c in range(*d_segs[seg]):
            pltpu.make_async_copy(wd_hbm.at[p, :, cols(c)], dbuf.at[c], d_sem.at[seg]).start()

    def wait_d(seg):
        lo, hi = d_segs[seg]
        ref = dbuf.at[pl.ds(lo, hi - lo)]
        pltpu.make_async_copy(ref, ref, d_sem.at[seg]).wait()

    for seg in range(3):
        start_gu(0, seg)
    for seg in range(3):
        start_d(0, seg)

    def slot_of(ids):
        ids = ids[...]
        e_iota = lax.broadcasted_iota(jnp.int32, (16, 128), 0)
        one0 = jnp.where(e_iota == ids[0:1, :], 1.0, 0.0).astype(F32)
        one1 = jnp.where(e_iota == ids[1:2, :], 1.0, 0.0).astype(F32)
        before = jnp.where(lax.broadcasted_iota(jnp.int32, (128, 128), 0)
                           < lax.broadcasted_iota(jnp.int32, (128, 128), 1), 1.0, 0.0)
        count = jnp.dot((one0 + one1).astype(BF16), before.astype(BF16), preferred_element_type=F32)
        rank0 = jnp.sum(one0 * count, axis=0, keepdims=True).astype(jnp.int32)
        rank1 = jnp.sum(one1 * count, axis=0, keepdims=True).astype(jnp.int32)
        return ids[0:1, :] * slots + rank0, ids[1:2, :] * slots + rank1

    def build(which, ids, gates):
        pos0, pos1 = slot_of(ids)
        k_iota = lax.broadcasted_iota(jnp.int32, (rows, 128), 0)
        hit0 = jnp.where(k_iota == pos0, 1.0, 0.0).astype(F32)
        hit1 = jnp.where(k_iota == pos1, 1.0, 0.0).astype(F32)
        picked = hit0 * gates[0:1, :] + hit1 * gates[1:2, :]
        gsel[which] = jnp.broadcast_to(jnp.sum(picked, axis=1, keepdims=True), (rows, CW))
        both = hit0 + hit1
        sel[which] = both.T.astype(BF16)
        return both.astype(BF16)

    in_copies[0].wait()
    in_copies[1].wait()
    gather = build(0, ids_ref, gate_ref)
    in_copies[2].wait()
    sorted_rows = jnp.dot(gather, xin[...], preferred_element_type=F32).astype(BF16)
    sendbuf[...] = sorted_rows.reshape(sendbuf.shape)
    for p in range(2):
        xbuf[p, tp, ep] = sendbuf[2 * ep + p]

    pl.semaphore_wait(barrier, 5)

    def row_copy(p, k):
        e, t = partners[k]
        return remote(sendbuf.at[2 * e + p], xbuf.at[p, tp, ep], xs_sem.at[p], xr_sem.at[p, (1, 2, 0, 0, 3)[k]], e, t)

    def relay_copy(p, k):
        home = (ex, exc)[k]
        return remote(xbuf.at[p, tp, home], xbuf.at[p, tp, home], xs_sem.at[2], xr_sem.at[p, 0], ep, tq)

    def wait_rows(p, k):
        ref = xbuf.at[p, tq] if k == 0 else xbuf.at[p, tp, (ex, exc, ec)[k - 1]]
        remote(ref, ref, xs_sem.at[0], xr_sem.at[p, k], ep, tq).wait_recv()

    def aux_copies():
        return (remote(ids_ref, ids_p, aux_s.at[0], aux_r.at[0], ep, tq),
                remote(gate_ref, gate_p, aux_s.at[1], aux_r.at[1], ep, tq))

    for k in range(5):
        row_copy(0, k).start()
    for k in (0, 1, 4):
        row_copy(1, k).start()
    for copy in aux_copies():
        copy.start()
    for k in range(2):
        wait_rows(0, 1 + k)
        relay_copy(0, k).start()
    for k in (2, 3):
        row_copy(1, k).start()
    wait_rows(0, 3)

    def y1_copy(p, cy):
        return remote(obuf.at[p, tq, cy], ybuf.at[p, cy], y1_sem.at[0], y1_sem.at[1], ep, tq)

    def x1_copy(p, g, cx, de, src_ep):
        th = tq if g else tp
        he = lax.rem(ep + de, 4)
        return remote(obuf.at[p, th, NY + cx, he], hx.at[g, cx, 2 * src_ep + p],
                      x1s_sem, x1r_sem.at[g, cx], he, tp)

    def y2_copy(p, cy, de, src_ep):
        he = lax.rem(ep + de, 4)
        return remote(ybuf.at[p, cy, he], hy.at[cy, 2 * src_ep + p],
                      y2s_sem, y2r_sem.at[cy], he, tp)

    def p_copy(cx):
        return remote(psend.at[cx], precv.at[cx], ps_sem, pr_sem.at[cx], ep, tq)

    def gate_up(p, g, wait=False, refill=False):
        th = tq if g else tp
        pieces = [(seg,) for seg in range(3)] if refill or (wait and p) else [tuple(range(3))]
        for piece in pieces:
            if wait:
                for seg in piece:
                    wait_gu(seg)
            xs = xbuf[p, th].reshape(half, xin.shape[1])
            for j in range(gu_segs[piece[0]][0], gu_segs[piece[-1]][1]):
                ab = jnp.dot(xs, gubuf[j], preferred_element_type=F32)
                a, b = ab[:, :CW], ab[:, CW:]
                hbuf[g, :, j * CW:(j + 1) * CW] = (jax.nn.silu(a) * b).astype(BF16)
            if refill:
                start_gu(1, piece[0])

    def down(p, g, seg, wait=False, refill=False):
        th = tq if g else tp
        if wait:
            wait_d(seg)
        for c in range(*d_segs[seg]):
            o = jnp.dot(hbuf[g], dbuf[c], preferred_element_type=F32)
            obuf[p, th, c] = o.reshape(4, slots, CW)
            if g and c < NY:
                y1_copy(p, c).start()
        for c in range(*d_segs[seg]):
            if c >= NY:
                for de in (2, 3, 1):
                    x1_copy(p, g, c - NY, de, ep).start()
                hx[g, c - NY, 2 * ep + p] = obuf[p, th, c, ep]
        if refill:
            start_d(1, seg)

    gate_up(0, 0, wait=True)
    for seg in range(3):
        down(0, 0, seg, wait=True)

    for k in range(2):
        wait_rows(1, 1 + k)
        relay_copy(1, k).start()
    wait_rows(0, 0)
    gate_up(0, 1, refill=True)
    for seg in range(3):
        down(0, 1, seg, refill=True)

    for copy in aux_copies():
        copy.wait_recv()
    build(1, ids_p, gate_p)
    wait_rows(1, 3)
    gate_up(1, 0, wait=True)
    down(1, 0, 0, wait=True)

    wait_rows(1, 0)
    gate_up(1, 1)
    down(1, 1, 2, wait=True)
    down(1, 1, 0)
    down(1, 1, 1, wait=True)

    down(1, 0, 1)
    down(1, 0, 2)

    def scatter(which, values):
        v = values.reshape(rows, CW) * gsel[which]
        hi = v.astype(BF16)
        rest = v - hi.astype(F32)
        mid = rest.astype(BF16)
        low = (rest - mid.astype(F32)).astype(BF16)
        s = sel[which]
        return (jnp.dot(s, low, preferred_element_type=F32)
                + jnp.dot(s, mid, preferred_element_type=F32)
                + jnp.dot(s, hi, preferred_element_type=F32))

    def wait_x(g, cx):
        six = hx.at[g, cx, pl.ds(0, 6)]
        remote(six, six, x1s_sem, x1r_sem.at[g, cx], ep, tq).wait_recv()

    def send_p(cx):
        wait_x(1, cx)
        psend[cx] = scatter(1, hx[1, cx])
        p_copy(cx).start()

    send_p(0)
    send_p(1)

    remote(ybuf, ybuf, y1_sem.at[0], y1_sem.at[1], ep, tq).wait_recv()

    @pl.loop(0, NY)
    def _(cy):
        for p in range(2):
            ybuf[p, cy] = ybuf[p, cy] + obuf[p, tp, cy]
            for de in (2, 3, 1):
                y2_copy(p, cy, de, ep).start()
            hy[cy, 2 * ep + p] = ybuf[p, cy, ep]

    @pl.loop(2, n_x)
    def _(cx):
        send_p(cx)

    @pl.loop(0, n_x)
    def _(cx):
        wait_x(0, cx)
        dacc[cx] = scatter(0, hx[0, cx])

    @pl.loop(0, n_x - 1)
    def _(cx):
        p_copy(cx).wait_recv()
        y_ref[:, cols(NY + cx)] = (dacc[cx] + precv[cx]).astype(y_ref.dtype)

    @pl.loop(0, NY)
    def _(cy):
        six = hy.at[cy, pl.ds(0, 6)]
        remote(six, six, y2s_sem, y2r_sem.at[cy], ep, tq).wait_recv()
        y_ref[:, cols(cy)] = scatter(0, hy[cy]).astype(y_ref.dtype)

    p_copy(n_x - 1).wait_recv()
    y_ref[:, cols(n_c - 1)] = (dacc[n_x - 1] + precv[n_x - 1]).astype(y_ref.dtype)

    for copy in aux_copies():
        copy.wait_send()
    for p in range(2):
        five = sendbuf.at[pl.ds(0, 5)]
        remote(five, five, xs_sem.at[p], xr_sem.at[0, 0], ep, tq).wait_send()
    four = xbuf.at[0, 0]
    remote(four, four, xs_sem.at[2], xr_sem.at[0, 0], ep, tq).wait_send()
    remote(ybuf, ybuf, y1_sem.at[0], y1_sem.at[1], ep, tq).wait_send()
    sent = hx.at[:, :, pl.ds(0, 6)]
    remote(sent, sent, x1s_sem, x1r_sem.at[0, 0], ep, tq).wait_send()
    sent = hy.at[:, pl.ds(0, 6)]
    remote(sent, sent, y2s_sem, y2r_sem.at[0], ep, tq).wait_send()
    remote(psend, psend, ps_sem, pr_sem.at[0], ep, tq).wait_send()


def solution(mesh):
    row_spec = P(('dp', 'ep', 'tp'), None)
    w_in_spec = P('ep', None, 'tp')
    w_out_spec = P('ep', 'tp', None)

    def local_moe(x_local, ids_local, gate_local, w_gate, w_up, w_down):
        n_rows, d_model = x_local.shape
        ff = w_gate.shape[2]
        slots = 2 * n_rows // 8
        n_gu = ff // CW
        n_c = d_model // CW
        n_x = n_c - NY
        dma = pltpu.SemaphoreType.DMA
        vmem = pl.BlockSpec(memory_space=pltpu.VMEM)
        hbm = pl.BlockSpec(memory_space=pltpu.HBM)
        return pl.pallas_call(
            moe_kernel,
            out_shape=jax.ShapeDtypeStruct((n_rows, d_model), BF16),
            in_specs=[hbm] * 6,
            out_specs=vmem,
            scratch_shapes=[
                pltpu.VMEM((2, n_rows), jnp.int32),
                pltpu.VMEM((2, n_rows), F32),
                pltpu.VMEM((n_rows, d_model), BF16),
                pltpu.VMEM((n_gu, d_model, 2 * CW), BF16),
                pltpu.VMEM((n_c, ff, CW), BF16),
                pltpu.VMEM((2, 2, 4, slots, d_model), BF16),
                pltpu.VMEM((8, slots, d_model), BF16),
                pltpu.VMEM((2, 4 * slots, ff), BF16),
                pltpu.VMEM((2, 2, n_c, 4, slots, CW), F32),
                pltpu.VMEM((2, NY, 4, slots, CW), F32),
                pltpu.VMEM((NY, 8, slots, CW), F32),
                pltpu.VMEM((2, n_x, 8, slots, CW), F32),
                pltpu.VMEM((n_x, n_rows, CW), F32),
                pltpu.VMEM((n_x, n_rows, CW), F32),
                pltpu.VMEM((n_x, n_rows, CW), F32),
                pltpu.VMEM((2, n_rows), jnp.int32),
                pltpu.VMEM((2, n_rows), F32),
                pltpu.VMEM((2, n_rows, 8 * slots), BF16),
                pltpu.VMEM((2, 8 * slots, CW), F32),
                dma((3,)), dma((3,)), dma((3,)),
                dma((3,)), dma((2, 4)), dma((2,)), dma((2,)),
                dma((2,)), dma, dma((2, n_x)),
                dma, dma((NY,)), dma, dma((n_x,)),
            ],
            compiler_params=pltpu.CompilerParams(
                collective_id=0, has_side_effects=True, vmem_limit_bytes=52 * 1024 * 1024),
        )(*(pltpu.with_memory_space_constraint(a, pltpu.HBM) for a in (ids_local.T, gate_local.T, x_local)),
          w_gate, w_up, w_down)

    return jax.shard_map(local_moe, mesh=mesh,
                         in_specs=(row_spec, row_spec, row_spec, w_in_spec, w_in_spec, w_out_spec),
                         out_specs=row_spec, check_vma=False)
```

```python
import jax
import jax.numpy as jnp
from jax import lax
from jax.experimental import pallas as pl
from jax.experimental.pallas import tpu as pltpu
from jax.sharding import PartitionSpec as P

MESH = pl.DeviceIdType.MESH
BF16 = jnp.bfloat16
F32 = jnp.float32
CW = 256
NY = 2


def moe_kernel(ids_hbm, gate_hbm, x_hbm, wg_hbm, wu_hbm, wd_hbm, y_ref,
               ids_ref, gate_ref, xin, gubuf, dbuf, xbuf, sendbuf, hbuf, obuf, ybuf, hy, hx, psend, precv, dacc,
               ids_p, gate_p, sel, gsel,
               in_sem, gu_sem, d_sem, out_sem, xr_sem, aux_sem,
               y1r_sem, x1r_sem, y2r_sem, pr_sem):
    n_gu = gubuf.shape[0]
    n_c = dbuf.shape[0]
    n_x = n_c - NY
    slots = sendbuf.shape[2]
    rows = 8 * slots
    half = 4 * slots
    ep = lax.axis_index('ep')
    tp = lax.axis_index('tp')
    tq = 1 - tp
    core = lax.rem(ep, 2)
    ec = ep + 1 - 2 * core
    ex = lax.rem(ep + 2, 4)
    exc = lax.rem(ec + 2, 4)

    def dev(e, t):
        return {'ep': e, 'tp': t}

    def cols(j):
        return pl.ds(pl.multiple_of(j * CW, CW), CW)

    def remote(src, dst, send, recv, e, t):
        return pltpu.make_async_remote_copy(src, dst, send, recv, device_id=dev(e, t), device_id_type=MESH)

    barrier = pltpu.get_barrier_semaphore()
    partners = ((ex, tp), (exc, tp), (ep, tq), (ec, tq), (ec, tp))
    for e, t in partners:
        pl.semaphore_signal(barrier, inc=1, device_id=dev(e, t), device_id_type=MESH)

    in_copies = [pltpu.make_async_copy(src, dst, in_sem.at[i // 2])
                 for i, (src, dst) in enumerate(((ids_hbm, ids_ref), (gate_hbm, gate_ref), (x_hbm, xin)))]
    for copy in in_copies:
        copy.start()

    def gu_copies(p, j, seg):
        return (pltpu.make_async_copy(wg_hbm.at[p, :, cols(j)], gubuf.at[j, :, pl.ds(0, CW)], gu_sem.at[seg]),
                pltpu.make_async_copy(wu_hbm.at[p, :, cols(j)], gubuf.at[j, :, pl.ds(CW, CW)], gu_sem.at[seg]))

    gu_segs = ((0, 4), (4, 8), (8, n_gu))
    d_segs = ((NY, NY + 1), (NY + 1, n_c), (0, NY))

    def start_gu(p, seg):
        @pl.loop(*gu_segs[seg])
        def _(j):
            for copy in gu_copies(p, j, seg):
                copy.start()

    def wait_gu(seg):
        lo, hi = gu_segs[seg]
        ref = gubuf.at[pl.ds(lo, hi - lo)]
        pltpu.make_async_copy(ref, ref, gu_sem.at[seg]).wait()

    def start_d(p, seg):
        for c in range(*d_segs[seg]):
            pltpu.make_async_copy(wd_hbm.at[p, :, cols(c)], dbuf.at[c], d_sem.at[seg]).start()

    def wait_d(seg):
        lo, hi = d_segs[seg]
        ref = dbuf.at[pl.ds(lo, hi - lo)]
        pltpu.make_async_copy(ref, ref, d_sem.at[seg]).wait()

    def slot_of(ids):
        ids = ids[...]
        e_iota = lax.broadcasted_iota(jnp.int32, (16, 128), 0)
        one0 = jnp.where(e_iota == ids[0:1, :], 1.0, 0.0).astype(F32)
        one1 = jnp.where(e_iota == ids[1:2, :], 1.0, 0.0).astype(F32)
        before = jnp.where(lax.broadcasted_iota(jnp.int32, (128, 128), 0)
                           < lax.broadcasted_iota(jnp.int32, (128, 128), 1), 1.0, 0.0)
        count = jnp.dot((one0 + one1).astype(BF16), before.astype(BF16), preferred_element_type=F32)
        rank0 = jnp.sum(one0 * count, axis=0, keepdims=True).astype(jnp.int32)
        rank1 = jnp.sum(one1 * count, axis=0, keepdims=True).astype(jnp.int32)
        return ids[0:1, :] * slots + rank0, ids[1:2, :] * slots + rank1

    def build(which, ids, gates):
        pos0, pos1 = slot_of(ids)
        k_iota = lax.broadcasted_iota(jnp.int32, (rows, 128), 0)
        hit0 = jnp.where(k_iota == pos0, 1.0, 0.0).astype(F32)
        hit1 = jnp.where(k_iota == pos1, 1.0, 0.0).astype(F32)
        picked = hit0 * gates[0:1, :] + hit1 * gates[1:2, :]
        gsel[which] = jnp.broadcast_to(jnp.sum(picked, axis=1, keepdims=True), (rows, CW))
        both = hit0 + hit1
        sel[which] = both.T.astype(BF16)

    def gather_rows(p, pos0, pos1):
        def place(ids, pos):
            return jnp.where(lax.rem(ids, 2) == p, pos - (ids // 2 + p) * slots, -1)
        ids = ids_ref[...]
        k_iota = lax.broadcasted_iota(jnp.int32, (half, 128), 0)
        hit0 = jnp.where(k_iota == place(ids[0:1, :], pos0), 1.0, 0.0).astype(F32)
        hit1 = jnp.where(k_iota == place(ids[1:2, :], pos1), 1.0, 0.0).astype(F32)
        picked = jnp.dot((hit0 + hit1).astype(BF16), xin[...], preferred_element_type=F32)
        sendbuf[p] = picked.astype(BF16).reshape(sendbuf.shape[1:])

    two = psend.at[0, pl.ds(0, 2)]
    pltpu.make_async_copy(two, two, in_sem.at[0]).wait()
    pos0, pos1 = slot_of(ids_ref)
    in_copies[2].wait()
    for seg in range(3):
        start_gu(0, seg)
    for seg in range(3):
        start_d(0, seg)
    gather_rows(0, pos0, pos1)
    pl.semaphore_wait(barrier, 5)

    def row_copy(p, k):
        e, t = partners[k]
        return remote(sendbuf.at[p, e], xbuf.at[p, tp, ep], out_sem, xr_sem.at[p, (1, 2, 0, 0, 2)[k]], e, t)

    def relay_copy(p, k):
        home = (ex, exc)[k]
        return remote(xbuf.at[p, tp, home], xbuf.at[p, tp, home], out_sem, xr_sem.at[p, 0], ep, tq)

    def wait_rows(p, k):
        ref = (xbuf.at[p, tq], sendbuf.at[0, 0], sendbuf.at[0, pl.ds(0, 2)])[k]
        remote(ref, ref, out_sem, xr_sem.at[p, k], ep, tq).wait_recv()

    def aux_copies():
        return (remote(ids_ref, ids_p, aux_sem.at[0], aux_sem.at[1], ep, tq),
                remote(gate_ref, gate_p, aux_sem.at[0], aux_sem.at[1], ep, tq))

    for k in range(5):
        row_copy(0, k).start()
    gather_rows(1, pos0, pos1)
    for k in (0, 1, 4):
        row_copy(1, k).start()
    for copy in aux_copies():
        copy.start()
    for p in range(2):
        xbuf[p, tp, ep] = sendbuf[p, ep]
    build(0, ids_ref, gate_ref)
    for k in range(2):
        wait_rows(0, 1 + k)
        relay_copy(0, k).start()
    for k in (2, 3):
        row_copy(1, k).start()

    def y1_copy(p, cy):
        return remote(obuf.at[p, tq, cy], ybuf.at[p, cy], out_sem, y1r_sem, ep, tq)

    def x1_copy(p, g, cx, de, src_ep):
        th = tq if g else tp
        he = lax.rem(ep + de, 4)
        return remote(obuf.at[p, th, NY + cx, he], hx.at[g, cx, 2 * src_ep + p],
                      out_sem, x1r_sem.at[cx if g else n_x], he, tp)

    def y2_copy(p, cy, he, src_ep):
        return remote(ybuf.at[p, cy, he], hy.at[cy, 2 * src_ep + p],
                      out_sem, y2r_sem.at[cy], he, tp)

    def p_copy(cx, last=0):
        return remote(psend.at[cx], precv.at[cx], out_sem, pr_sem.at[last], ep, tq)

    def gate_up(p, g, wait=False, refill=False):
        th = tq if g else tp
        pieces = [(seg,) for seg in range(3)] if refill or (wait and p) else [tuple(range(3))]
        for piece in pieces:
            if wait:
                for seg in piece:
                    wait_gu(seg)
            xs = xbuf[p, th].reshape(half, xin.shape[1])
            for j in range(gu_segs[piece[0]][0], gu_segs[piece[-1]][1]):
                ab = jnp.dot(xs, gubuf[j], preferred_element_type=F32)
                a, b = ab[:, :CW], ab[:, CW:]
                hbuf[g, :, j * CW:(j + 1) * CW] = (jax.nn.silu(a) * b).astype(BF16)
            if refill:
                start_gu(1, piece[0])

    def down(p, g, seg, wait=False, refill=False):
        th = tq if g else tp
        if wait:
            wait_d(seg)
        for c in range(*d_segs[seg]):
            o = jnp.dot(hbuf[g], dbuf[c], preferred_element_type=F32)
            obuf[p, th, c] = o.reshape(4, slots, CW)
            if g and c < NY:
                y1_copy(p, c).start()
        for c in range(*d_segs[seg]):
            if c >= NY:
                for de in (2, 3, 1):
                    x1_copy(p, g, c - NY, de, ep).start()
                hx[g, c - NY, 2 * ep + p] = obuf[p, th, c, ep]
        if refill:
            start_d(1, seg)

    gate_up(0, 0, wait=True)
    for seg in range(3):
        down(0, 0, seg, wait=True)

    for k in range(2):
        wait_rows(1, 1 + k)
        relay_copy(1, k).start()
    wait_rows(0, 0)
    gate_up(0, 1, refill=True)
    for seg in range(3):
        down(0, 1, seg, refill=True)

    remote(two, two, aux_sem.at[0], aux_sem.at[1], ep, tq).wait_recv()
    build(1, ids_p, gate_p)
    gate_up(1, 0, wait=True)
    down(1, 0, 0, wait=True)

    wait_rows(1, 0)
    gate_up(1, 1)
    down(1, 1, 2, wait=True)
    down(1, 1, 0)
    down(1, 1, 1, wait=True)

    down(1, 0, 1)
    down(1, 0, 2)

    def scatter(which, values):
        v = values.reshape(rows, CW) * gsel[which]
        hi = v.astype(BF16)
        rest = v - hi.astype(F32)
        mid = rest.astype(BF16)
        low = (rest - mid.astype(F32)).astype(BF16)
        s = sel[which]
        return (jnp.dot(s, low, preferred_element_type=F32)
                + jnp.dot(s, mid, preferred_element_type=F32)
                + jnp.dot(s, hi, preferred_element_type=F32))

    def wait_x(cx):
        six = hx.at[1, cx, pl.ds(0, 6)]
        remote(six, six, out_sem, x1r_sem.at[cx], ep, tq).wait_recv()

    def send_p(cx, last=0):
        wait_x(cx)
        psend[cx] = scatter(1, hx[1, cx])
        if last < 2:
            p_copy(cx, last).start()

    send_p(0)
    send_p(1)

    remote(ybuf, ybuf, out_sem, y1r_sem, ep, tq).wait_recv()

    @pl.loop(0, NY)
    def _(cy):
        for p in range(2):
            ybuf[p, cy] = ybuf[p, cy] + obuf[p, tp, cy]
            for he in (ex - core, ec):
                y2_copy(p, cy, he, ep).start()
            hy[cy, 2 * ep + p] = ybuf[p, cy, ep]

    @pl.loop(0, NY)
    def _(cy):
        for p in range(2):
            y2_copy(p, cy, ex - core + 1, ep).start()

    send_p(2)
    for cx in range(3, n_x):
        send_p(cx, 2)

    def send_rest():
        for cx in range(3, n_x - 1):
            p_copy(cx, 1).start()
        p_copy(n_x - 1, 2).start()

    def wait_first():
        first = precv.at[pl.ds(0, 3)]
        remote(first, first, out_sem, pr_sem.at[0], ep, tq).wait_recv()

    @pl.when(core == 0)
    def _():
        send_rest()

    @pl.when(core == 1)
    def _():
        wait_first()
        send_rest()

    sixes = hx.at[0, :, pl.ds(0, 6)]
    remote(sixes, sixes, out_sem, x1r_sem.at[n_x], ep, tq).wait_recv()

    @pl.loop(0, n_x)
    def _(cx):
        dacc[cx] = scatter(0, hx[0, cx])

    @pl.when(core == 0)
    def _():
        wait_first()

    early = precv.at[pl.ds(3, n_x - 4)]
    remote(early, early, out_sem, pr_sem.at[1], ep, tq).wait_recv()

    @pl.loop(0, n_x - 1)
    def _(cx):
        y_ref[:, cols(NY + cx)] = (dacc[cx] + precv[cx]).astype(y_ref.dtype)

    @pl.loop(0, NY)
    def _(cy):
        six = hy.at[cy, pl.ds(0, 6)]
        remote(six, six, out_sem, y2r_sem.at[cy], ep, tq).wait_recv()
        y_ref[:, cols(cy)] = scatter(0, hy[cy]).astype(y_ref.dtype)

    p_copy(n_x - 1, 2).wait_recv()
    y_ref[:, cols(n_c - 1)] = (dacc[n_x - 1] + precv[n_x - 1]).astype(y_ref.dtype)

    remote(two, two, aux_sem.at[0], aux_sem.at[1], ep, tq).wait_send()
    sent = gubuf.at[pl.ds(0, 5), pl.ds(0, 1152)]
    remote(sent, sent, out_sem, pr_sem.at[0], ep, tq).wait_send()


def solution(mesh):
    row_spec = P(('dp', 'ep', 'tp'), None)
    w_in_spec = P('ep', None, 'tp')
    w_out_spec = P('ep', 'tp', None)

    def local_moe(x_local, ids_local, gate_local, w_gate, w_up, w_down):
        n_rows, d_model = x_local.shape
        ff = w_gate.shape[2]
        slots = 2 * n_rows // 8
        n_gu = ff // CW
        n_c = d_model // CW
        n_x = n_c - NY
        dma = pltpu.SemaphoreType.DMA
        vmem = pl.BlockSpec(memory_space=pltpu.VMEM)
        hbm = pl.BlockSpec(memory_space=pltpu.HBM)
        return pl.pallas_call(
            moe_kernel,
            out_shape=jax.ShapeDtypeStruct((n_rows, d_model), BF16),
            in_specs=[hbm] * 6,
            out_specs=vmem,
            scratch_shapes=[
                pltpu.VMEM((2, n_rows), jnp.int32),
                pltpu.VMEM((2, n_rows), F32),
                pltpu.VMEM((n_rows, d_model), BF16),
                pltpu.VMEM((n_gu, d_model, 2 * CW), BF16),
                pltpu.VMEM((n_c, ff, CW), BF16),
                pltpu.VMEM((2, 2, 4, slots, d_model), BF16),
                pltpu.VMEM((2, 4, slots, d_model), BF16),
                pltpu.VMEM((2, 4 * slots, ff), BF16),
                pltpu.VMEM((2, 2, n_c, 4, slots, CW), F32),
                pltpu.VMEM((2, NY, 4, slots, CW), F32),
                pltpu.VMEM((NY, 8, slots, CW), F32),
                pltpu.VMEM((2, n_x, 8, slots, CW), F32),
                pltpu.VMEM((n_x, n_rows, CW), F32),
                pltpu.VMEM((n_x, n_rows, CW), F32),
                pltpu.VMEM((n_x, n_rows, CW), F32),
                pltpu.VMEM((2, n_rows), jnp.int32),
                pltpu.VMEM((2, n_rows), F32),
                pltpu.VMEM((2, n_rows, 8 * slots), BF16),
                pltpu.VMEM((2, 8 * slots, CW), F32),
                dma((2,)), dma((3,)), dma((3,)),
                dma, dma((2, 3)), dma((2,)),
                dma, dma((n_x + 1,)), dma((NY,)), dma((3,)),
            ],
            compiler_params=pltpu.CompilerParams(
                collective_id=0, has_side_effects=True, vmem_limit_bytes=52 * 1024 * 1024),
        )(*(pltpu.with_memory_space_constraint(a, pltpu.HBM) for a in (ids_local.T, gate_local.T, x_local)),
          w_gate, w_up, w_down)

    return jax.shard_map(local_moe, mesh=mesh,
                         in_specs=(row_spec, row_spec, row_spec, w_in_spec, w_in_spec, w_out_spec),
                         out_specs=row_spec, check_vma=False)
```

```python
import jax
import jax.numpy as jnp
from jax import lax
from jax.experimental import pallas as pl
from jax.experimental.pallas import tpu as pltpu
from jax.sharding import PartitionSpec as P

MESH = pl.DeviceIdType.MESH
BF16 = jnp.bfloat16
F32 = jnp.float32
F32_MAX = float(jnp.finfo(F32).max)
BF16_MAX = float(jnp.finfo(BF16).max)
CW = 256
NY = 2


def moe_kernel(ids_hbm, gate_hbm, x_hbm, wg_hbm, wu_hbm, wd_hbm, y_ref,
               ids_ref, gate_ref, xin, gubuf, dbuf, xbuf, sendbuf, hbuf, obuf, ybuf, hy, hx, psend, precv, dacc,
               ids_p, gate_p, sel, gsel,
               in_sem, gu_sem, d_sem, out_sem, xr_sem, aux_sem,
               y1r_sem, x1r_sem, y2r_sem, pr_sem):
    n_gu = gubuf.shape[0]
    n_c = dbuf.shape[0]
    n_x = n_c - NY
    slots = sendbuf.shape[2]
    rows = 8 * slots
    half = 4 * slots
    ep = lax.axis_index('ep')
    tp = lax.axis_index('tp')
    tq = 1 - tp
    core = lax.rem(ep, 2)
    ec = ep + 1 - 2 * core
    ex = lax.rem(ep + 2, 4)
    exc = lax.rem(ec + 2, 4)

    def dev(e, t):
        return {'ep': e, 'tp': t}

    def cols(j):
        return pl.ds(pl.multiple_of(j * CW, CW), CW)

    def remote(src, dst, send, recv, e, t):
        return pltpu.make_async_remote_copy(src, dst, send, recv, device_id=dev(e, t), device_id_type=MESH)

    barrier = pltpu.get_barrier_semaphore()
    partners = ((ex, tp), (exc, tp), (ep, tq), (ec, tq), (ec, tp))
    for e, t in partners:
        pl.semaphore_signal(barrier, inc=1, device_id=dev(e, t), device_id_type=MESH)

    in_copies = [pltpu.make_async_copy(src, dst, in_sem.at[i // 2])
                 for i, (src, dst) in enumerate(((ids_hbm, ids_ref), (gate_hbm, gate_ref), (x_hbm, xin)))]
    for copy in in_copies:
        copy.start()

    def gu_copies(p, j, seg):
        return (pltpu.make_async_copy(wg_hbm.at[p, :, cols(j)], gubuf.at[j, :, pl.ds(0, CW)], gu_sem.at[seg]),
                pltpu.make_async_copy(wu_hbm.at[p, :, cols(j)], gubuf.at[j, :, pl.ds(CW, CW)], gu_sem.at[seg]))

    gu_segs = ((0, 4), (4, 8), (8, n_gu))
    d_segs = ((NY, NY + 1), (NY + 1, n_c), (0, NY))

    def start_gu(p, seg):
        @pl.loop(*gu_segs[seg])
        def _(j):
            for copy in gu_copies(p, j, seg):
                copy.start()

    def wait_gu(seg):
        lo, hi = gu_segs[seg]
        ref = gubuf.at[pl.ds(lo, hi - lo)]
        pltpu.make_async_copy(ref, ref, gu_sem.at[seg]).wait()

    def start_d(p, seg):
        for c in range(*d_segs[seg]):
            pltpu.make_async_copy(wd_hbm.at[p, :, cols(c)], dbuf.at[c], d_sem.at[seg]).start()

    def wait_d(seg):
        lo, hi = d_segs[seg]
        ref = dbuf.at[pl.ds(lo, hi - lo)]
        pltpu.make_async_copy(ref, ref, d_sem.at[seg]).wait()

    def slot_of(ids):
        ids = ids[...]
        e_iota = lax.broadcasted_iota(jnp.int32, (16, 128), 0)
        one0 = jnp.where(e_iota == ids[0:1, :], 1.0, 0.0).astype(F32)
        one1 = jnp.where(e_iota == ids[1:2, :], 1.0, 0.0).astype(F32)
        before = jnp.where(lax.broadcasted_iota(jnp.int32, (128, 128), 0)
                           < lax.broadcasted_iota(jnp.int32, (128, 128), 1), 1.0, 0.0)
        count = jnp.dot((one0 + one1).astype(BF16), before.astype(BF16), preferred_element_type=F32)
        rank0 = jnp.sum(one0 * count, axis=0, keepdims=True).astype(jnp.int32)
        rank1 = jnp.sum(one1 * count, axis=0, keepdims=True).astype(jnp.int32)
        return ids[0:1, :] * slots + rank0, ids[1:2, :] * slots + rank1

    def build(which, ids, gates):
        pos0, pos1 = slot_of(ids)
        k_iota = lax.broadcasted_iota(jnp.int32, (rows, 128), 0)
        hit0 = jnp.where(k_iota == pos0, 1.0, 0.0).astype(F32)
        hit1 = jnp.where(k_iota == pos1, 1.0, 0.0).astype(F32)
        picked = hit0 * gates[0:1, :] + hit1 * gates[1:2, :]
        gsel[which] = jnp.broadcast_to(jnp.sum(picked, axis=1, keepdims=True), (rows, CW))
        both = hit0 + hit1
        sel[which] = both.T.astype(BF16)

    def gather_rows(p, pos0, pos1):
        def place(ids, pos):
            return jnp.where(lax.rem(ids, 2) == p, pos - (ids // 2 + p) * slots, -1)
        ids = ids_ref[...]
        k_iota = lax.broadcasted_iota(jnp.int32, (half, 128), 0)
        hit0 = jnp.where(k_iota == place(ids[0:1, :], pos0), 1.0, 0.0).astype(F32)
        hit1 = jnp.where(k_iota == place(ids[1:2, :], pos1), 1.0, 0.0).astype(F32)
        picked = jnp.dot((hit0 + hit1).astype(BF16), xin[...], preferred_element_type=F32)
        sendbuf[p] = picked.astype(BF16).reshape(sendbuf.shape[1:])

    two = psend.at[0, pl.ds(0, 2)]
    pltpu.make_async_copy(two, two, in_sem.at[0]).wait()
    pos0, pos1 = slot_of(ids_ref)
    in_copies[2].wait()
    for seg in range(3):
        start_gu(0, seg)
    for seg in range(3):
        start_d(0, seg)
    gather_rows(0, pos0, pos1)
    pl.semaphore_wait(barrier, 5)

    def row_copy(p, k):
        e, t = partners[k]
        return remote(sendbuf.at[p, e], xbuf.at[p, tp, ep], out_sem, xr_sem.at[p, (1, 2, 0, 0, 2)[k]], e, t)

    def relay_copy(p, k):
        home = (ex, exc)[k]
        return remote(xbuf.at[p, tp, home], xbuf.at[p, tp, home], out_sem, xr_sem.at[p, 0], ep, tq)

    def wait_rows(p, k):
        ref = (xbuf.at[p, tq], sendbuf.at[0, 0], sendbuf.at[0, pl.ds(0, 2)])[k]
        remote(ref, ref, out_sem, xr_sem.at[p, k], ep, tq).wait_recv()

    def aux_copies():
        return (remote(ids_ref, ids_p, aux_sem.at[0], aux_sem.at[1], ep, tq),
                remote(gate_ref, gate_p, aux_sem.at[0], aux_sem.at[1], ep, tq))

    for k in range(5):
        row_copy(0, k).start()
    gather_rows(1, pos0, pos1)
    for k in (0, 1, 4):
        row_copy(1, k).start()
    for copy in aux_copies():
        copy.start()
    for p in range(2):
        xbuf[p, tp, ep] = sendbuf[p, ep]
    build(0, ids_ref, gate_ref)
    for k in range(2):
        wait_rows(0, 1 + k)
        relay_copy(0, k).start()
    for k in (2, 3):
        row_copy(1, k).start()

    def y1_copy(p, cy):
        return remote(obuf.at[p, tq, cy], ybuf.at[p, cy], out_sem, y1r_sem, ep, tq)

    def x1_copy(p, g, cx, de, src_ep):
        th = tq if g else tp
        he = lax.rem(ep + de, 4)
        return remote(obuf.at[p, th, NY + cx, he], hx.at[g, cx, 2 * src_ep + p],
                      out_sem, x1r_sem.at[cx if g else n_x], he, tp)

    def y2_copy(p, cy, he, src_ep):
        return remote(ybuf.at[p, cy, he], hy.at[cy, 2 * src_ep + p],
                      out_sem, y2r_sem.at[cy], he, tp)

    def p_copy(cx, last=0):
        return remote(psend.at[cx], precv.at[cx], out_sem, pr_sem.at[last], ep, tq)

    def gate_up(p, g, wait=False, refill=False):
        th = tq if g else tp
        pieces = [(seg,) for seg in range(3)] if refill or (wait and p) else [tuple(range(3))]
        for piece in pieces:
            if wait:
                for seg in piece:
                    wait_gu(seg)
            xs = xbuf[p, th].reshape(half, xin.shape[1])
            for j in range(gu_segs[piece[0]][0], gu_segs[piece[-1]][1]):
                ab = jnp.dot(xs, gubuf[j], preferred_element_type=F32)
                a, b = ab[:, :CW], ab[:, CW:]
                hbuf[g, :, j * CW:(j + 1) * CW] = (jax.nn.silu(a) * b).astype(BF16)
            if refill:
                start_gu(1, piece[0])

    def down(p, g, seg, wait=False, refill=False):
        th = tq if g else tp
        if wait:
            wait_d(seg)
        for c in range(*d_segs[seg]):
            o = jnp.dot(hbuf[g], dbuf[c], preferred_element_type=F32)
            obuf[p, th, c] = o.reshape(4, slots, CW)
            if g and c < NY:
                y1_copy(p, c).start()
        for c in range(*d_segs[seg]):
            if c >= NY:
                for de in (2, 3, 1):
                    x1_copy(p, g, c - NY, de, ep).start()
                hx[g, c - NY, 2 * ep + p] = obuf[p, th, c, ep]
        if refill:
            start_d(1, seg)

    gate_up(0, 0, wait=True)
    for seg in range(3):
        down(0, 0, seg, wait=True)

    for k in range(2):
        wait_rows(1, 1 + k)
        relay_copy(1, k).start()
    wait_rows(0, 0)
    gate_up(0, 1, refill=True)
    for seg in range(3):
        down(0, 1, seg, refill=True)

    remote(two, two, aux_sem.at[0], aux_sem.at[1], ep, tq).wait_recv()
    build(1, ids_p, gate_p)
    gate_up(1, 0, wait=True)
    down(1, 0, 0, wait=True)

    wait_rows(1, 0)
    gate_up(1, 1)
    down(1, 1, 2, wait=True)
    down(1, 1, 0)
    down(1, 1, 1, wait=True)

    down(1, 0, 1)
    down(1, 0, 2)

    def scatter(which, values):
        v = jnp.clip(values.reshape(rows, CW) * gsel[which], -F32_MAX, F32_MAX)
        hi = jnp.clip(v, -BF16_MAX, BF16_MAX).astype(BF16)
        rest = v - hi.astype(F32)
        mid = rest.astype(BF16)
        low = (rest - mid.astype(F32)).astype(BF16)
        s = sel[which]
        return (jnp.dot(s, low, preferred_element_type=F32)
                + jnp.dot(s, mid, preferred_element_type=F32)
                + jnp.dot(s, hi, preferred_element_type=F32))

    def wait_x(cx):
        six = hx.at[1, cx, pl.ds(0, 6)]
        remote(six, six, out_sem, x1r_sem.at[cx], ep, tq).wait_recv()

    def send_p(cx, last=0):
        wait_x(cx)
        psend[cx] = scatter(1, hx[1, cx])
        if last < 2:
            p_copy(cx, last).start()

    send_p(0)
    send_p(1)

    remote(ybuf, ybuf, out_sem, y1r_sem, ep, tq).wait_recv()

    @pl.loop(0, NY)
    def _(cy):
        for p in range(2):
            ybuf[p, cy] = ybuf[p, cy] + obuf[p, tp, cy]
            for he in (ex - core, ec):
                y2_copy(p, cy, he, ep).start()
            hy[cy, 2 * ep + p] = ybuf[p, cy, ep]

    @pl.loop(0, NY)
    def _(cy):
        for p in range(2):
            y2_copy(p, cy, ex - core + 1, ep).start()

    send_p(2)
    for cx in range(3, n_x):
        send_p(cx, 2)

    def send_rest():
        for cx in range(3, n_x - 1):
            p_copy(cx, 1).start()
        p_copy(n_x - 1, 2).start()

    def wait_first():
        first = precv.at[pl.ds(0, 3)]
        remote(first, first, out_sem, pr_sem.at[0], ep, tq).wait_recv()

    @pl.when(core == 0)
    def _():
        send_rest()

    @pl.when(core == 1)
    def _():
        wait_first()
        send_rest()

    sixes = hx.at[0, :, pl.ds(0, 6)]
    remote(sixes, sixes, out_sem, x1r_sem.at[n_x], ep, tq).wait_recv()

    @pl.loop(0, n_x)
    def _(cx):
        dacc[cx] = scatter(0, hx[0, cx])

    @pl.when(core == 0)
    def _():
        wait_first()

    early = precv.at[pl.ds(3, n_x - 4)]
    remote(early, early, out_sem, pr_sem.at[1], ep, tq).wait_recv()

    @pl.loop(0, n_x - 1)
    def _(cx):
        y_ref[:, cols(NY + cx)] = (dacc[cx] + precv[cx]).astype(y_ref.dtype)

    @pl.loop(0, NY)
    def _(cy):
        six = hy.at[cy, pl.ds(0, 6)]
        remote(six, six, out_sem, y2r_sem.at[cy], ep, tq).wait_recv()
        y_ref[:, cols(cy)] = scatter(0, hy[cy]).astype(y_ref.dtype)

    p_copy(n_x - 1, 2).wait_recv()
    y_ref[:, cols(n_c - 1)] = (dacc[n_x - 1] + precv[n_x - 1]).astype(y_ref.dtype)

    remote(two, two, aux_sem.at[0], aux_sem.at[1], ep, tq).wait_send()
    sent = gubuf.at[pl.ds(0, 5), pl.ds(0, 1152)]
    remote(sent, sent, out_sem, pr_sem.at[0], ep, tq).wait_send()


def solution(mesh):
    row_spec = P(('dp', 'ep', 'tp'), None)
    w_in_spec = P('ep', None, 'tp')
    w_out_spec = P('ep', 'tp', None)

    def local_moe(x_local, ids_local, gate_local, w_gate, w_up, w_down):
        n_rows, d_model = x_local.shape
        ff = w_gate.shape[2]
        slots = 2 * n_rows // 8
        n_gu = ff // CW
        n_c = d_model // CW
        n_x = n_c - NY
        dma = pltpu.SemaphoreType.DMA
        vmem = pl.BlockSpec(memory_space=pltpu.VMEM)
        hbm = pl.BlockSpec(memory_space=pltpu.HBM)
        return pl.pallas_call(
            moe_kernel,
            out_shape=jax.ShapeDtypeStruct((n_rows, d_model), BF16),
            in_specs=[hbm] * 6,
            out_specs=vmem,
            scratch_shapes=[
                pltpu.VMEM((2, n_rows), jnp.int32),
                pltpu.VMEM((2, n_rows), F32),
                pltpu.VMEM((n_rows, d_model), BF16),
                pltpu.VMEM((n_gu, d_model, 2 * CW), BF16),
                pltpu.VMEM((n_c, ff, CW), BF16),
                pltpu.VMEM((2, 2, 4, slots, d_model), BF16),
                pltpu.VMEM((2, 4, slots, d_model), BF16),
                pltpu.VMEM((2, 4 * slots, ff), BF16),
                pltpu.VMEM((2, 2, n_c, 4, slots, CW), F32),
                pltpu.VMEM((2, NY, 4, slots, CW), F32),
                pltpu.VMEM((NY, 8, slots, CW), F32),
                pltpu.VMEM((2, n_x, 8, slots, CW), F32),
                pltpu.VMEM((n_x, n_rows, CW), F32),
                pltpu.VMEM((n_x, n_rows, CW), F32),
                pltpu.VMEM((n_x, n_rows, CW), F32),
                pltpu.VMEM((2, n_rows), jnp.int32),
                pltpu.VMEM((2, n_rows), F32),
                pltpu.VMEM((2, n_rows, 8 * slots), BF16),
                pltpu.VMEM((2, 8 * slots, CW), F32),
                dma((2,)), dma((3,)), dma((3,)),
                dma, dma((2, 3)), dma((2,)),
                dma, dma((n_x + 1,)), dma((NY,)), dma((3,)),
            ],
            compiler_params=pltpu.CompilerParams(
                collective_id=0, has_side_effects=True, vmem_limit_bytes=52 * 1024 * 1024),
        )(*(pltpu.with_memory_space_constraint(a, pltpu.HBM) for a in (ids_local.T, gate_local.T, x_local)),
          w_gate, w_up, w_down)

    return jax.shard_map(local_moe, mesh=mesh,
                         in_specs=(row_spec, row_spec, row_spec, w_in_spec, w_in_spec, w_out_spec),
                         out_specs=row_spec, check_vma=False)
```

```python
import jax
import jax.numpy as jnp
from jax import lax
from jax.experimental import pallas as pl
from jax.experimental.pallas import tpu as pltpu
from jax.sharding import PartitionSpec as P

MESH = pl.DeviceIdType.MESH
BF16 = jnp.bfloat16
F32 = jnp.float32
F32_MAX = float(jnp.finfo(F32).max)
BF16_MAX = float(jnp.finfo(BF16).max)
CW = 256
NY = 2


def moe_kernel(ids_hbm, gate_hbm, x_hbm, wg_hbm, wu_hbm, wd_hbm, y_ref,
               ids_ref, gate_ref, xin, gubuf, dbuf, xbuf, sendbuf, hbuf, obuf, ybuf, hy, hx, psend, precv, dacc,
               ids_p, gate_p, sel, gsel,
               in_sem, gu_sem, d_sem, out_sem, xr_sem, aux_sem,
               y1r_sem, x1r_sem, y2r_sem, pr_sem):
    n_gu = gubuf.shape[0]
    n_c = dbuf.shape[0]
    n_x = n_c - NY
    slots = sendbuf.shape[2]
    rows = 8 * slots
    half = 4 * slots
    ep = lax.axis_index('ep')
    tp = lax.axis_index('tp')
    tq = 1 - tp
    core = lax.rem(ep, 2)
    ec = ep + 1 - 2 * core
    ex = lax.rem(ep + 2, 4)
    exc = lax.rem(ec + 2, 4)

    def dev(e, t):
        return {'ep': e, 'tp': t}

    def cols(j):
        return pl.ds(pl.multiple_of(j * CW, CW), CW)

    def remote(src, dst, send, recv, e, t):
        return pltpu.make_async_remote_copy(src, dst, send, recv, device_id=dev(e, t), device_id_type=MESH)

    barrier = pltpu.get_barrier_semaphore()
    partners = ((ex, tp), (exc, tp), (ep, tq), (ec, tq), (ec, tp))
    for e, t in partners:
        pl.semaphore_signal(barrier, inc=1, device_id=dev(e, t), device_id_type=MESH)

    in_copies = [pltpu.make_async_copy(src, dst, in_sem.at[i // 2])
                 for i, (src, dst) in enumerate(((ids_hbm, ids_ref), (gate_hbm, gate_ref), (x_hbm, xin)))]
    for copy in in_copies:
        copy.start()

    def gu_copies(p, j, seg):
        return (pltpu.make_async_copy(wg_hbm.at[p, :, cols(j)], gubuf.at[j, :, pl.ds(0, CW)], gu_sem.at[seg]),
                pltpu.make_async_copy(wu_hbm.at[p, :, cols(j)], gubuf.at[j, :, pl.ds(CW, CW)], gu_sem.at[seg]))

    gu_segs = ((0, 4), (4, 8), (8, n_gu))
    d_segs = ((NY, NY + 1), (NY + 1, n_c), (0, NY))

    def start_gu(p, seg):
        @pl.loop(*gu_segs[seg])
        def _(j):
            for copy in gu_copies(p, j, seg):
                copy.start()

    def wait_gu(seg):
        lo, hi = gu_segs[seg]
        ref = gubuf.at[pl.ds(lo, hi - lo)]
        pltpu.make_async_copy(ref, ref, gu_sem.at[seg]).wait()

    def start_d(p, seg):
        for c in range(*d_segs[seg]):
            pltpu.make_async_copy(wd_hbm.at[p, :, cols(c)], dbuf.at[c], d_sem.at[seg]).start()

    def wait_d(seg):
        lo, hi = d_segs[seg]
        ref = dbuf.at[pl.ds(lo, hi - lo)]
        pltpu.make_async_copy(ref, ref, d_sem.at[seg]).wait()

    def slot_of(ids):
        ids = ids[...]
        e_iota = lax.broadcasted_iota(jnp.int32, (16, 128), 0)
        one0 = jnp.where(e_iota == ids[0:1, :], 1.0, 0.0).astype(F32)
        one1 = jnp.where(e_iota == ids[1:2, :], 1.0, 0.0).astype(F32)
        before = jnp.where(lax.broadcasted_iota(jnp.int32, (128, 128), 0)
                           < lax.broadcasted_iota(jnp.int32, (128, 128), 1), 1.0, 0.0)
        count = jnp.dot((one0 + one1).astype(BF16), before.astype(BF16), preferred_element_type=F32)
        rank0 = jnp.sum(one0 * count, axis=0, keepdims=True).astype(jnp.int32)
        rank1 = jnp.sum(one1 * count, axis=0, keepdims=True).astype(jnp.int32)
        return ids[0:1, :] * slots + rank0, ids[1:2, :] * slots + rank1

    def build(which, ids, gates):
        pos0, pos1 = slot_of(ids)
        k_iota = lax.broadcasted_iota(jnp.int32, (rows, 128), 0)
        hit0 = jnp.where(k_iota == pos0, 1.0, 0.0).astype(F32)
        hit1 = jnp.where(k_iota == pos1, 1.0, 0.0).astype(F32)
        picked = hit0 * gates[0:1, :] + hit1 * gates[1:2, :]
        gsel[which] = jnp.broadcast_to(jnp.sum(picked, axis=1, keepdims=True), (rows, CW))
        both = hit0 + hit1
        sel[which] = both.T.astype(BF16)

    def gather_rows(p, pos0, pos1):
        def place(ids, pos):
            return jnp.where(lax.rem(ids, 2) == p, pos - (ids // 2 + p) * slots, -1)
        ids = ids_ref[...]
        k_iota = lax.broadcasted_iota(jnp.int32, (half, 128), 0)
        hit0 = jnp.where(k_iota == place(ids[0:1, :], pos0), 1.0, 0.0).astype(F32)
        hit1 = jnp.where(k_iota == place(ids[1:2, :], pos1), 1.0, 0.0).astype(F32)
        picked = jnp.dot((hit0 + hit1).astype(BF16), xin[...], preferred_element_type=F32)
        sendbuf[p] = picked.astype(BF16).reshape(sendbuf.shape[1:])

    two = psend.at[0, pl.ds(0, 2)]
    pltpu.make_async_copy(two, two, in_sem.at[0]).wait()
    pos0, pos1 = slot_of(ids_ref)
    in_copies[2].wait()
    for seg in range(3):
        start_gu(0, seg)
    for seg in range(3):
        start_d(0, seg)
    gather_rows(0, pos0, pos1)
    pl.semaphore_wait(barrier, 5)

    def row_copy(p, k):
        e, t = partners[k]
        return remote(sendbuf.at[p, e], xbuf.at[p, tp, ep], out_sem, xr_sem.at[p, (1, 2, 0, 0, 2)[k]], e, t)

    def relay_copy(p, k):
        home = (ex, exc)[k]
        return remote(xbuf.at[p, tp, home], xbuf.at[p, tp, home], out_sem, xr_sem.at[p, 0], ep, tq)

    def wait_rows(p, k):
        ref = (xbuf.at[p, tq], sendbuf.at[0, 0], sendbuf.at[0, pl.ds(0, 2)])[k]
        remote(ref, ref, out_sem, xr_sem.at[p, k], ep, tq).wait_recv()

    def aux_copies():
        return (remote(ids_ref, ids_p, aux_sem.at[0], aux_sem.at[1], ep, tq),
                remote(gate_ref, gate_p, aux_sem.at[0], aux_sem.at[1], ep, tq))

    for k in range(5):
        row_copy(0, k).start()
    gather_rows(1, pos0, pos1)
    for k in (0, 1, 4):
        row_copy(1, k).start()
    for copy in aux_copies():
        copy.start()
    for p in range(2):
        xbuf[p, tp, ep] = sendbuf[p, ep]
    build(0, ids_ref, gate_ref)
    for k in range(2):
        wait_rows(0, 1 + k)
        relay_copy(0, k).start()
    for k in (2, 3):
        row_copy(1, k).start()

    def y1_copy(p, cy):
        return remote(obuf.at[p, tq, cy], ybuf.at[p, cy], out_sem, y1r_sem, ep, tq)

    def x1_copy(p, g, cx, de, src_ep):
        th = tq if g else tp
        he = lax.rem(ep + de, 4)
        return remote(obuf.at[p, th, NY + cx, he], hx.at[g, cx, 2 * src_ep + p],
                      out_sem, x1r_sem.at[cx if g else n_x], he, tp)

    def y2_copy(p, cy, he, src_ep):
        return remote(ybuf.at[p, cy, he], hy.at[cy, 2 * src_ep + p],
                      out_sem, y2r_sem.at[cy], he, tp)

    def p_copy(cx, last=0):
        return remote(psend.at[cx], precv.at[cx], out_sem, pr_sem.at[last], ep, tq)

    def gate_up(p, g, wait=False, refill=False):
        th = tq if g else tp
        pieces = [(seg,) for seg in range(3)] if refill or (wait and p) else [tuple(range(3))]
        for piece in pieces:
            if wait:
                for seg in piece:
                    wait_gu(seg)
            xs = xbuf[p, th].reshape(half, xin.shape[1])
            for j in range(gu_segs[piece[0]][0], gu_segs[piece[-1]][1]):
                ab = jnp.dot(xs, gubuf[j], preferred_element_type=F32)
                a, b = ab[:, :CW], ab[:, CW:]
                hbuf[g, :, j * CW:(j + 1) * CW] = (jax.nn.silu(a) * b).astype(BF16)
            if refill:
                start_gu(1, piece[0])

    def down(p, g, seg, wait=False, refill=False):
        th = tq if g else tp
        if wait:
            wait_d(seg)
        for c in range(*d_segs[seg]):
            o = jnp.dot(hbuf[g], dbuf[c], preferred_element_type=F32)
            obuf[p, th, c] = o.reshape(4, slots, CW)
            if g and c < NY:
                y1_copy(p, c).start()
        for c in range(*d_segs[seg]):
            if c >= NY:
                for de in (2, 3, 1):
                    x1_copy(p, g, c - NY, de, ep).start()
                hx[g, c - NY, 2 * ep + p] = obuf[p, th, c, ep]
        if refill:
            start_d(1, seg)

    gate_up(0, 0, wait=True)
    for seg in range(3):
        down(0, 0, seg, wait=True)

    for k in range(2):
        wait_rows(1, 1 + k)
        relay_copy(1, k).start()
    wait_rows(0, 0)
    gate_up(0, 1, refill=True)
    for seg in range(3):
        down(0, 1, seg, refill=True)

    remote(two, two, aux_sem.at[0], aux_sem.at[1], ep, tq).wait_recv()
    build(1, ids_p, gate_p)
    gate_up(1, 0, wait=True)
    down(1, 0, 0, wait=True)

    wait_rows(1, 0)
    gate_up(1, 1)
    down(1, 1, 2, wait=True)
    down(1, 1, 0)
    down(1, 1, 1, wait=True)

    down(1, 0, 1)
    down(1, 0, 2)

    def scatter(which, values):
        v = jnp.clip(values.reshape(rows, CW) * gsel[which], -F32_MAX, F32_MAX)
        hi = jnp.clip(v, -BF16_MAX, BF16_MAX).astype(BF16)
        rest = v - hi.astype(F32)
        mid = rest.astype(BF16)
        low = (rest - mid.astype(F32)).astype(BF16)
        s = sel[which]
        return (jnp.dot(s, low, preferred_element_type=F32)
                + jnp.dot(s, mid, preferred_element_type=F32)
                + jnp.dot(s, hi, preferred_element_type=F32))

    def wait_x(cx):
        six = hx.at[1, cx, pl.ds(0, 6)]
        remote(six, six, out_sem, x1r_sem.at[cx], ep, tq).wait_recv()

    def send_p(cx, last=0):
        wait_x(cx)
        psend[cx] = scatter(1, hx[1, cx])
        if last < 2:
            p_copy(cx, last).start()

    send_p(0)
    send_p(1)

    remote(ybuf, ybuf, out_sem, y1r_sem, ep, tq).wait_recv()

    @pl.loop(0, NY)
    def _(cy):
        for p in range(2):
            ybuf[p, cy] = ybuf[p, cy] + obuf[p, tp, cy]
            for he in (ex - core, ec):
                y2_copy(p, cy, he, ep).start()
            hy[cy, 2 * ep + p] = ybuf[p, cy, ep]

    @pl.loop(0, NY)
    def _(cy):
        for p in range(2):
            y2_copy(p, cy, ex - core + 1, ep).start()

    for cx in range(2, n_x):
        send_p(cx, 2)

    def send_rest():
        for cx in range(2, n_x - 1):
            p_copy(cx, 1).start()
        p_copy(n_x - 1, 2).start()

    def wait_first():
        first = precv.at[pl.ds(0, 2)]
        remote(first, first, out_sem, pr_sem.at[0], ep, tq).wait_recv()

    @pl.when(core == 0)
    def _():
        send_rest()

    @pl.when(core == 1)
    def _():
        wait_first()
        send_rest()

    sixes = hx.at[0, :, pl.ds(0, 6)]
    remote(sixes, sixes, out_sem, x1r_sem.at[n_x], ep, tq).wait_recv()

    @pl.loop(0, n_x)
    def _(cx):
        dacc[cx] = scatter(0, hx[0, cx])

    @pl.when(core == 0)
    def _():
        wait_first()

    early = precv.at[pl.ds(2, n_x - 3)]
    remote(early, early, out_sem, pr_sem.at[1], ep, tq).wait_recv()

    @pl.loop(0, n_x - 1)
    def _(cx):
        y_ref[:, cols(NY + cx)] = (dacc[cx] + precv[cx]).astype(y_ref.dtype)

    @pl.loop(0, NY)
    def _(cy):
        six = hy.at[cy, pl.ds(0, 6)]
        remote(six, six, out_sem, y2r_sem.at[cy], ep, tq).wait_recv()
        y_ref[:, cols(cy)] = scatter(0, hy[cy]).astype(y_ref.dtype)

    p_copy(n_x - 1, 2).wait_recv()
    y_ref[:, cols(n_c - 1)] = (dacc[n_x - 1] + precv[n_x - 1]).astype(y_ref.dtype)

    remote(two, two, aux_sem.at[0], aux_sem.at[1], ep, tq).wait_send()
    sent = gubuf.at[pl.ds(0, 5), pl.ds(0, 1152)]
    remote(sent, sent, out_sem, pr_sem.at[0], ep, tq).wait_send()


def solution(mesh):
    row_spec = P(('dp', 'ep', 'tp'), None)
    w_in_spec = P('ep', None, 'tp')
    w_out_spec = P('ep', 'tp', None)

    def local_moe(x_local, ids_local, gate_local, w_gate, w_up, w_down):
        n_rows, d_model = x_local.shape
        ff = w_gate.shape[2]
        slots = 2 * n_rows // 8
        n_gu = ff // CW
        n_c = d_model // CW
        n_x = n_c - NY
        dma = pltpu.SemaphoreType.DMA
        vmem = pl.BlockSpec(memory_space=pltpu.VMEM)
        hbm = pl.BlockSpec(memory_space=pltpu.HBM)
        return pl.pallas_call(
            moe_kernel,
            out_shape=jax.ShapeDtypeStruct((n_rows, d_model), BF16),
            in_specs=[hbm] * 6,
            out_specs=vmem,
            scratch_shapes=[
                pltpu.VMEM((2, n_rows), jnp.int32),
                pltpu.VMEM((2, n_rows), F32),
                pltpu.VMEM((n_rows, d_model), BF16),
                pltpu.VMEM((n_gu, d_model, 2 * CW), BF16),
                pltpu.VMEM((n_c, ff, CW), BF16),
                pltpu.VMEM((2, 2, 4, slots, d_model), BF16),
                pltpu.VMEM((2, 4, slots, d_model), BF16),
                pltpu.VMEM((2, 4 * slots, ff), BF16),
                pltpu.VMEM((2, 2, n_c, 4, slots, CW), F32),
                pltpu.VMEM((2, NY, 4, slots, CW), F32),
                pltpu.VMEM((NY, 8, slots, CW), F32),
                pltpu.VMEM((2, n_x, 8, slots, CW), F32),
                pltpu.VMEM((n_x, n_rows, CW), F32),
                pltpu.VMEM((n_x, n_rows, CW), F32),
                pltpu.VMEM((n_x, n_rows, CW), F32),
                pltpu.VMEM((2, n_rows), jnp.int32),
                pltpu.VMEM((2, n_rows), F32),
                pltpu.VMEM((2, n_rows, 8 * slots), BF16),
                pltpu.VMEM((2, 8 * slots, CW), F32),
                dma((2,)), dma((3,)), dma((3,)),
                dma, dma((2, 3)), dma((2,)),
                dma, dma((n_x + 1,)), dma((NY,)), dma((3,)),
            ],
            compiler_params=pltpu.CompilerParams(
                collective_id=0, has_side_effects=True, vmem_limit_bytes=52 * 1024 * 1024),
        )(*(pltpu.with_memory_space_constraint(a, pltpu.HBM) for a in (ids_local.T, gate_local.T, x_local)),
          w_gate, w_up, w_down)

    return jax.shard_map(local_moe, mesh=mesh,
                         in_specs=(row_spec, row_spec, row_spec, w_in_spec, w_in_spec, w_out_spec),
                         out_specs=row_spec, check_vma=False)
```
